512 devices in a mesh: group: 8 (over y), shard: 64 (over z, x, core).
Axes of the slice: x: 4, y: 8, z: 8, core: 2. Of those that a mesh axis runs over, the one named last changes fastest.
Arguments:
- item_features: bfloat16 [65536, 1024], P(('group', 'shard')), may hold values from -24 to 24
- tower_weight: bfloat16 [1024, 1024], replicated, may hold values from -0.1875 to 0.1875
- item_table: bfloat16 [65536, 1024], P(('group', 'shard')), may hold values from -4 to 4
- owner: int32 [65536, 1], P(('group', 'shard')), may hold values from 0 to 63; in each aligned block of 128 rows (0 to 127, 128 to 255, ...) at most 4 rows name the same one
- table_slot: int32 [65536], P(('group', 'shard')), may hold values from 0 to 127
- pair_users: int32 [65536, 2], P(('group', 'shard')), may hold values from 0 to 255
- user_comps: bfloat16 [2048, 1024], P(('group', 'shard')), may hold values from -0.5 to 0.5
- user_gates: bfloat16 [2048, 64], P(('group', 'shard')), may hold values from -6 to 6
Outputs:
- tower_grad: float32 [1024, 1024], P('shard')
- table_grad: float32 [65536, 1024], P(('group', 'shard'))
- user_comp_grad: float32 [2048, 1024], P(('group', 'shard'))
- user_gate_grad: float32 [2048, 64], P(('group', 'shard'))
The draws below stay inside these ranges and needn't reach their ends.
Inputs may be any that keep to these rules, and one draw needn't show every extreme that they name: Among the rows of one device, no owner is named more than 4 times, a bound that some block reaches. `pair_users`: user numbers within the item's own group.
All inputs are finite; a program needn't handle non-finite values.
Results may differ from the reference program's by a relative error of at most 0.0042.
Values may be sent and summed in bfloat16 or wider, within the bound.
A program may use at most 64 MiB of HBM per device.

```python
import math
import jax
import jax.numpy as jnp
import numpy as np
from jax import lax

COMPS = 8
D = 1024
ITEM_DEV = 128
TABLE_DEV = 128
CAP = 4
USERS_G = 256
ITEMS = 65536
TABLE = 65536
USERS = 2048
N_GROUP = 8
N_SHARD = 64


def touch_ends(values, stream_key, low, top_value):
    spot = [jax.random.randint(jax.random.fold_in(stream_key, axis), (), 0, length) for axis, length in enumerate(values.shape)]
    main_axis = values.shape.index(max(values.shape))
    beside = spot[:main_axis] + [(spot[main_axis] + 1) % values.shape[main_axis]] + spot[main_axis + 1:]
    return values.at[tuple(spot)].set(low).at[tuple(beside)].set(top_value)


def strengthened(drawn, stream_key, source, target, parts, factor):
    def block_of(dim):
        return (jnp.arange(drawn.shape[dim]) // (drawn.shape[dim] // parts)).reshape((-1,) + (1,) * (drawn.ndim - 1 - dim))

    first = jax.random.permutation(stream_key, parts)[block_of(target)]
    far = (block_of(target) + parts // 2) % parts
    return jnp.where((block_of(source) == first) | (block_of(source) == far), factor * drawn, drawn)


def level_of(own_key, extent, split, low, high):
    gain, own = 1.0, jax.random.fold_in(own_key, 6)
    for dim, blocks in split:
        heights = jnp.exp(jax.random.uniform(jax.random.fold_in(own, dim), (blocks,), jnp.float32, low / len(split), high / len(split)))
        gain = gain * jnp.repeat(heights, extent[dim] // blocks).reshape([-1 if axis == dim else 1 for axis in range(len(extent))])
    return gain


def deal_out(own_key, own, number, rows, number_of, top, reach, skew):
    ranking = jax.random.permutation(own_key, number_of)
    packed, common = shares(number_of, rows * top, reach, skew, True), shares(number_of, rows * top, reach, skew, False)
    places = jnp.arange(number_of)

    def named(tallies, turn):
        used = int((tallies > 0).sum())
        fixed = max(1, used // 4)
        moved = fixed + (places - fixed + turn * (used - fixed)) % max(1, number_of - fixed)
        return jnp.zeros((number_of,), jnp.int32).at[ranking[jnp.where(places < fixed, places, moved)]].set(jnp.asarray(tallies, jnp.int32))

    tallies = jnp.where(number % 4 == 0, named(packed, number // 4), named(common, number - number // 4 - 1))
    mixed = jax.random.permutation(jax.random.fold_in(own, 3), number_of)
    giver, sink = mixed[0:number_of // 2 * 2:2], mixed[1:number_of // 2 * 2:2]
    room = jnp.minimum(tallies[giver] - 1, reach - tallies[sink]) // 2
    room = jnp.where((giver == ranking[0]) | (sink == ranking[0]) | (tallies[sink] == 0), 0, jnp.maximum(room, 0))
    moved = jax.random.randint(jax.random.fold_in(own, 4), (number_of // 2,), 0, 1 << 20) % (room + 1)
    tallies = tallies.at[giver].add(-moved).at[sink].add(moved)
    items = jnp.searchsorted(jnp.cumsum(tallies), jnp.arange(rows * top), side="right").astype(jnp.int32)
    listing = items.reshape(top, rows).T
    listing = listing[jax.random.permutation(jax.random.fold_in(own, 1), rows)]
    turn = jax.random.randint(jax.random.fold_in(own, 2), (rows, 1), 0, top)
    return jnp.take_along_axis(listing, (jnp.arange(top)[None, :] + turn) % top, axis=1)


def shares(count, total, bound, skew, full):
    loads = [(1 << 20) // math.isqrt(grade ** skew) + 1 for grade in range(1, count + 1)]
    largest = bound if full else min(bound, max(-(-total // count), total * loads[0] // sum(loads)))
    least = 1 if total - largest >= count - 1 else 0
    counts, surplus = [largest] + [least] * (count - 1), total - largest - least * (count - 1)
    while surplus > 0:
        candidates = [i for i in range(1, count) if counts[i] < largest] or [i for i in range(1, count) if counts[i] < bound]
        mass, left = sum([loads[i] for i in candidates]), surplus
        for i in candidates:
            extra = min(bound - counts[i], max(1, left * loads[i] // mass), surplus)
            counts[i] = counts[i] + extra
            surplus = surplus - extra
    return np.array(counts)


def centred(rng, extent, width, limit, shards=(), kind=jnp.bfloat16):
    drawn = width * jax.random.normal(rng, extent, jnp.float32)
    if shards:
        drawn = drawn * level_of(rng, extent, shards, -0.22, 0.18)
    return jnp.clip(drawn, -limit, limit).astype(kind)


def gaussian_with(own_key, shape, scale, reach, split, heavy, dtype=jnp.bfloat16):
    array = scale * jax.random.normal(own_key, shape, jnp.float32)
    if split:
        array = array * level_of(own_key, shape, split, -0.22, 0.18)
    return jnp.clip(strengthened(array, jax.random.fold_in(own_key, 3), *heavy), -reach, reach).astype(dtype)


def setup_inputs(seed: int = 0) -> dict:
    key_of = jax.random.split(jax.random.key(seed), 9)
    item_features = gaussian_with(key_of[0], (ITEMS, D), 1.0, 24.0, ((0, 512),), (0, 1, 512, 6.0))
    tower_weight = centred(key_of[1], (D, D), D ** -0.5, 0.1875)
    item_table = centred(key_of[2], (TABLE, D), 0.6, 4.0, ((0, 512),))
    owner_keys = jax.random.split(jax.random.fold_in(key_of[3], 1), ITEMS // ITEM_DEV)
    owner_turns = jax.random.permutation(jax.random.fold_in(key_of[3], 3), ITEMS // ITEM_DEV)
    owner = jax.vmap(lambda own, number: deal_out(jax.random.fold_in(key_of[3], 2), own, number, ITEM_DEV, N_SHARD, 1, CAP, 2))(owner_keys, owner_turns).reshape((ITEMS, 1))
    table_slot = touch_ends(jax.random.randint(key_of[4], (ITEMS,), 0, TABLE_DEV), jax.random.fold_in(key_of[4], 1), 0, TABLE_DEV - 1).astype(jnp.int32)
    pair_users = touch_ends(jax.random.randint(key_of[5], (ITEMS, 2), 0, USERS_G), jax.random.fold_in(key_of[5], 1), 0, USERS_G - 1).astype(jnp.int32)
    user_comps = centred(key_of[6], (USERS, D), 0.09, 0.5, ((0, 512),))
    user_gates = centred(key_of[7], (USERS, COMPS * COMPS), 1.5, 6.0, ((0, 512),))
    return dict(item_features=item_features, tower_weight=tower_weight, item_table=item_table, owner=owner, table_slot=table_slot, pair_users=pair_users, user_comps=user_comps, user_gates=user_gates)


highest = lax.Precision.HIGHEST

def exact_gelu(values):
    return jax.nn.gelu(values, approximate=False)

def mixture_score(normed, users, gates):
    rows_here = normed.shape[0]
    logits = jnp.einsum('npk,nqk->npq', users, normed, precision=highest)
    weights = jax.nn.sigmoid(gates.reshape(rows_here, COMPS, COMPS) + logits)
    return 0.125 * lax.optimization_barrier(jnp.sum(weights * logits, axis=(1, 2)))

def pair_loss(embedded, table_rows, pos_users, neg_users, pos_gates, neg_gates, present):
    rows_here = embedded.shape[0]
    combined = (embedded + table_rows).reshape(rows_here, COMPS, -1)
    normed = combined * lax.rsqrt(lax.optimization_barrier(jnp.mean(combined * combined, axis=-1, keepdims=True)) + 1e-06)
    pos_score = mixture_score(normed, pos_users.reshape(rows_here, COMPS, -1), pos_gates)
    neg_score = mixture_score(normed, neg_users.reshape(rows_here, COMPS, -1), neg_gates)
    return jnp.sum(present * (jax.nn.softplus(-pos_score) + jax.nn.softplus(neg_score)))

def reference(item_features, tower_weight, item_table, owner, table_slot, pair_users, user_comps, user_gates):
    group_items = ITEM_DEV * N_SHARD
    group_table = TABLE_DEV * N_SHARD
    gate_width = COMPS * COMPS

    def one_group(carry, stacked):
        features, targets, slot_ids, pairs, table, users, gates = stacked
        preact = jnp.dot(features, tower_weight, preferred_element_type=jnp.float32)
        gelu_value, gelu_back = jax.vjp(exact_gelu, preact)
        embedded = lax.optimization_barrier(gelu_value.astype(jnp.bfloat16)).astype(jnp.float32)
        table_index = (targets[:, 0] * TABLE_DEV + slot_ids).astype(jnp.int32)
        pos_ids = pairs[:, 0]
        neg_ids = pairs[:, 1]
        table_rows = table[table_index].astype(jnp.float32)
        pos_users = users[pos_ids].astype(jnp.float32)
        neg_users = users[neg_ids].astype(jnp.float32)
        pos_gates = gates[pos_ids].astype(jnp.float32)
        neg_gates = gates[neg_ids].astype(jnp.float32)
        present = jnp.ones((group_items,), jnp.float32)
        derivs = jax.grad(pair_loss, argnums=(0, 1, 2, 3, 4, 5))(embedded, table_rows, pos_users, neg_users, pos_gates, neg_gates, present)
        table_grad = jnp.zeros((group_table, D), jnp.float32).at[table_index].add(derivs[1])
        user_grad = jnp.zeros((USERS_G, D), jnp.float32).at[pos_ids].add(derivs[2]).at[neg_ids].add(derivs[3])
        gate_grad = jnp.zeros((USERS_G, gate_width), jnp.float32).at[pos_ids].add(derivs[4]).at[neg_ids].add(derivs[5])
        rounded = lax.optimization_barrier(derivs[0].astype(jnp.bfloat16)).astype(jnp.float32)
        d_preact = gelu_back(rounded)[0].astype(jnp.bfloat16)
        carry = carry + lax.dot_general(features, d_preact, (((0,), (0,)), ((), ())), preferred_element_type=jnp.float32)
        return (carry, (table_grad, user_grad, gate_grad))
    stacked = (item_features.reshape(N_GROUP, group_items, D), owner.reshape(N_GROUP, group_items, 1), table_slot.reshape(N_GROUP, group_items), pair_users.reshape(N_GROUP, group_items, 2), item_table.reshape(N_GROUP, group_table, D), user_comps.reshape(N_GROUP, USERS_G, D), user_gates.reshape(N_GROUP, USERS_G, gate_width))
    tower_grad, outputs = lax.scan(one_group, jnp.zeros((D, D), jnp.float32), stacked)
    table_grads, user_grads, gate_grads = outputs
    return (tower_grad, table_grads.reshape(-1, D), user_grads.reshape(-1, D), gate_grads.reshape(-1, gate_width))
```

```python
import functools

import jax
import jax.numpy as jnp
from jax import lax
from jax.experimental import pallas as pl
from jax.experimental.pallas import tpu as pltpu
from jax.sharding import PartitionSpec as P

MESH = pl.DeviceIdType.MESH
COMPS = 8
CAP = 4
CORES = 2
QUARTERS = 4
BLOCK = CAP * QUARTERS
GROUP = 16
LANES = 128
F32, BF16 = jnp.float32, jnp.bfloat16


def nn(a, b):
    return lax.dot_general(a, b, (((1,), (0,)), ((), ())), preferred_element_type=F32)


def nt(a, b):
    return lax.dot_general(a, b, (((1,), (1,)), ((), ())), preferred_element_type=F32)


def tn(a, b):
    return lax.dot_general(a, b, (((0,), (0,)), ((), ())), preferred_element_type=F32)


def ones_where(condition):
    return jnp.where(condition, 1.0, 0.0).astype(BF16)


def iota(shape, dim):
    return lax.broadcasted_iota(jnp.int32, shape, dim)


def halves(values):
    high = values.astype(BF16)
    return high, (values - high.astype(F32)).astype(BF16)


def sigmoid(values):
    return 1.0 / (1.0 + jnp.exp(-values))


def kernel(
    groups, shards, nx,
    ids_ref, x_ref, w_ref, table_ref, own_users_ref,
    tower_out, table_out, users_out, gates_out,
    head_send, head_recv, users_all, xt, xt_recv, embedded, slope, rows_send, rows_recv,
    picked, gates_wide, combined, d_comb, d_pre, d_pre_recv, d_users, d_gates,
    users_part, users_part_recv, tower_part, tower_x, tower_mid, tower_z, tower_low, tower_y,
    users_half, users_x, users_mid, users_z, back_send, back_recv,
    send_sems, recv_sems,
):
    n, d = x_ref.shape
    slots = table_ref.shape[0]
    width = d // QUARTERS
    rows = shards * BLOCK
    half = rows // CORES
    nz = shards // (nx * CORES)
    depth = d // shards
    chips = shards // CORES
    g, s = lax.axis_index("group"), lax.axis_index("shard")
    core = lax.rem(s, CORES)
    chip = lax.div(s, CORES)
    x, z = lax.rem(chip, nx), lax.div(chip, nx)

    def at(z_to, x_to, core_to):
        return (g, (z_to * nx + x_to) * CORES + core_to)

    partner = at(z, x, 1 - core)

    def copy(number, source, target, device):
        return pltpu.make_async_remote_copy(
            src_ref=source, dst_ref=target,
            send_sem=send_sems.at[number], recv_sem=recv_sems.at[number],
            device_id=device, device_id_type=MESH,
        )

    def wait_recv(number, whole):
        copy(number, whole, whole, partner).wait_recv()

    def wait_send(number, whole):
        copy(number, whole, whole, partner).wait_send()

    def loop(low, high, step):
        def run(i, carry):
            step(i)
            return carry
        lax.fori_loop(low, high, run, 0)

    def block(i, size):
        return pl.ds(pl.multiple_of(i * size, size), size)

    barrier = pltpu.get_barrier_semaphore()
    loop(1, shards, lambda k: pl.semaphore_signal(
        barrier, inc=1, device_id=(g, lax.rem(s + k, shards)), device_id_type=MESH))
    loop(1, groups, lambda k: pl.semaphore_signal(
        barrier, inc=1, device_id=(lax.rem(g + k, groups), s), device_id_type=MESH))

    target = ids_ref[0:1, :]
    slot = ids_ref[1:2, :]
    to_owner = jnp.where(iota((shards, n), 0) == target, 1.0, 0.0)
    earlier = ones_where(iota((n, n), 0) < iota((n, n), 1))
    before = nn(to_owner.astype(BF16), earlier)
    within = jnp.sum(before * to_owner, axis=0, keepdims=True).astype(jnp.int32)
    place_row = (target * CAP + within) * QUARTERS
    eye = iota((n, n), 0) == iota((n, n), 1)

    def as_column(row):
        wide = jnp.where(eye, row.astype(F32), 0.0)
        return jnp.sum(wide, axis=1, keepdims=True).astype(jnp.int32)

    place_col = as_column(place_row)
    wanted = (to_owner * (slot + 1).astype(F32)).astype(BF16)
    turn = ones_where(iota((LANES, n), 0) == within)
    head_send[...] = nt(wanted, turn).reshape(shards, 1, LANES)

    for tile in range(d // LANES):
        turned = x_ref[:, tile * LANES:(tile + 1) * LANES].astype(F32).T.astype(BF16)
        for piece in range(max(1, LANES // depth)):
            size = min(depth, LANES)
            first = tile * LANES + piece * size
            holder, rest = divmod(first, depth)
            c_h, chip_h = holder % CORES, holder // CORES
            row = ((chip_h % nx) * nz + chip_h // nx) * depth + rest
            xt[c_h, row:row + size, :] = turned[piece * size:(piece + 1) * size]

    own = core * chips + x * nz + z
    users_all[block(own, BLOCK), :] = own_users_ref[...]

    pl.semaphore_wait(barrier, shards - 1 + groups - 1)

    def send_head(k):
        p = lax.rem(s + k, shards)
        copy(0, head_send.at[p], head_recv.at[s], (g, p)).start()
    loop(1, shards, send_head)
    head_recv[s] = head_send[s]

    def send_users(k):
        p = lax.rem(chip + k, chips)
        copy(1, own_users_ref, users_all.at[block(own, BLOCK)], (g, p * CORES + core)).start()
    loop(1, chips, send_users)
    copy(2, xt.at[1 - core], xt_recv, partner).start()

    def tower(q):
        columns = block(q, width)
        pre = nn(x_ref[...], w_ref[:, columns])
        share = 0.5 + 0.5 * lax.erf(pre * (0.5 ** 0.5))
        embedded[block(q, n), :] = (pre * share).astype(BF16)
        slope[:, columns] = share + pre * (0.3989422804014327 * jnp.exp(-0.5 * pre * pre))
    loop(0, QUARTERS, tower)

    wait_recv(0, head_recv.at[pl.ds(0, shards - 1)])
    heads = head_recv[...].reshape(shards, LANES).astype(BF16)

    tile_rows = min(256, rows)

    def answer(t):
        index = iota((tile_rows, shards), 0) + t * tile_rows
        spread = nn(ones_where((index >> 4) == iota((tile_rows, shards), 1)), heads)
        index = iota((tile_rows, LANES), 0) + t * tile_rows
        mine = jnp.where(((index >> 2) & 3) == iota((tile_rows, LANES), 1), spread, 0.0)
        asked = jnp.sum(mine, axis=1, keepdims=True).astype(jnp.int32) - 1
        quarter = index[:, 0:1] & 3
        out = jnp.zeros((tile_rows, width), F32)
        for q in range(QUARTERS):
            key = jnp.where(quarter == q, asked, -1)
            pick = ones_where(key == iota((tile_rows, slots), 1))
            out = out + nn(pick, table_ref[:, q * width:(q + 1) * width])
        rows_send[block(t, tile_rows), :] = out.astype(BF16)
    loop(0, rows // tile_rows, answer)

    def send_rows(k):
        p = lax.rem(s + k, shards)
        copy(3, rows_send.at[block(p, BLOCK)], rows_recv.at[block(s, BLOCK)], (g, p)).start()
    loop(1, shards, send_rows)
    rows_recv[block(s, BLOCK), :] = rows_send[block(s, BLOCK), :]

    others = pl.ds(0, half - BLOCK)
    wait_recv(1, users_all.at[others])
    mine = pl.ds(pl.multiple_of(core * half, half), half)
    copy(4, users_all.at[mine], users_all.at[mine], partner).start()

    held = tn(heads, ones_where((iota((shards, rows), 1) >> 4) == iota((shards, rows), 0)))
    lane = iota((LANES, rows), 1)
    held = jnp.where(((lane >> 2) & 3) == iota((LANES, rows), 0), held, 0.0)
    asked_row = jnp.sum(held, axis=0, keepdims=True).astype(jnp.int32) - 1

    def user_key(row):
        user, holder = row & 3, row >> 2
        c_u, chip_u = holder & 1, holder >> 1
        where = c_u * chips + (chip_u & (nx - 1)) * nz + (chip_u >> (nx.bit_length() - 1))
        return (where * CAP + user) * QUARTERS

    key_rows = [user_key(ids_ref[2 + side:3 + side, :]) for side in range(2)]
    key_cols = [as_column(row) for row in key_rows]
    expand = ones_where(iota((LANES, width), 0) == (iota((LANES, width), 1) >> 4))
    wait_recv(4, users_all.at[mine])
    for side in range(2):
        def pick_users(q):
            pick = ones_where(key_cols[side] + q == iota((n, rows), 1))
            got = nn(pick, users_all[...]).astype(BF16)
            here = block(side * QUARTERS + q, n)
            picked[here, :] = got[:, :width]
            gates_wide[here, :] = nn(got[:, width:], expand).astype(BF16)
        loop(0, QUARTERS, pick_users)

    wait_recv(3, rows_recv.at[pl.ds(0, rows - BLOCK)])

    def combine(q):
        pick = ones_where(place_col + q == iota((n, rows), 1))
        here = block(q, n)
        combined[here, :] = embedded[here, :].astype(F32) + nn(pick, rows_recv[...])
    loop(0, QUARTERS, combine)

    def spot(index, b):
        return pl.ds(pl.multiple_of(index * n + b * GROUP, GROUP), GROUP)

    def lanes_of(p):
        return slice((p & 1) * LANES, (p & 1) * LANES + LANES)

    def stack(ref, b, sides):
        return jnp.concatenate(
            [ref[spot(side * QUARTERS + (p >> 1), b), lanes_of(p)] for side in range(sides) for p in range(COMPS)],
            axis=0)

    pairs = COMPS * GROUP

    def pair_loss(b):
        comb = stack(combined, b, 1)
        scale = lax.rsqrt(jnp.mean(comb * comb, axis=1, keepdims=True) + 1e-06)
        normed = comb * scale
        n_high, n_low = halves(normed)
        users = stack(picked, b, 2)
        gates = stack(gates_wide, b, 2).astype(F32)
        logits = nt(users, n_high) + nt(users, n_low)
        same = (iota((2 * pairs, pairs), 0) & (GROUP - 1)) == (iota((2 * pairs, pairs), 1) & (GROUP - 1))
        weights = sigmoid(gates + logits)
        terms = jnp.where(same, weights * logits, 0.0)
        factors = []
        for side in range(2):
            total = terms[side * pairs:side * pairs + GROUP]
            for p in range(1, COMPS):
                total = total + terms[side * pairs + p * GROUP:side * pairs + (p + 1) * GROUP]
            score = 0.125 * jnp.sum(total, axis=1, keepdims=True)
            factor = sigmoid(score) if side else -sigmoid(-score)
            factors += [0.125 * factor] * COMPS
        factor = jnp.where(same, jnp.concatenate(factors, axis=0), 0.0)
        bend = logits * (weights * (1.0 - weights))
        dg_high, dg_low = halves(factor * bend)
        dl = factor * (weights + bend)
        dl_high, dl_low = halves(dl)
        d_normed = tn(dl_high, users) + tn(dl_low, users)
        du_high, du_low = halves(nn(dl_high, n_high) + nn(dl_low, n_high) + nn(dl_high, n_low))
        d_row = scale * (d_normed - normed * jnp.mean(d_normed * normed, axis=1, keepdims=True))
        d_row = d_row.astype(BF16)
        for p in range(COMPS):
            part = d_row[p * GROUP:(p + 1) * GROUP]
            d_comb[spot(p >> 1, b), lanes_of(p)] = part
            item, column = block(b, GROUP), slice(p * LANES, (p + 1) * LANES)
            d_pre[item, column] = (part.astype(F32) * slope[item, column]).astype(BF16)
        for side in range(2):
            for p in range(COMPS):
                here = spot(side * QUARTERS + (p >> 1), b)
                part = slice(side * pairs + p * GROUP, side * pairs + (p + 1) * GROUP)
                lane0 = (p & 1) * LANES
                d_users[here, lane0:lane0 + LANES] = du_high[part]
                d_users[here, width + lane0:width + lane0 + LANES] = du_low[part]
                d_gates[here, lane0:lane0 + LANES] = dg_high[part]
                d_gates[here, width + lane0:width + lane0 + LANES] = dg_low[part]
    loop(0, n // GROUP, pair_loss)

    copy(5, d_pre, d_pre_recv, partner).start()

    def give_back(t):
        index = iota((tile_rows, n), 0) + t * tile_rows
        put = jnp.concatenate([ones_where(index == place_row + q) for q in range(QUARTERS)], axis=1)
        back_send[block(t, tile_rows), :] = nn(put, d_comb[...]).astype(BF16)
    loop(0, rows // tile_rows, give_back)

    def send_back(k):
        p = lax.rem(s + k, shards)
        copy(6, back_send.at[block(p, BLOCK)], back_recv.at[block(s, BLOCK)], (g, p)).start()
    loop(1, shards, send_back)
    back_recv[block(s, BLOCK), :] = back_send[block(s, BLOCK), :]

    wait_recv(2, xt_recv)
    wait_recv(5, d_pre_recv)
    wide = nz * depth

    def tower_rows(i):
        here = block(i, wide)
        total = nn(xt[core, here, :], d_pre[...]) + nn(xt_recv[here, :], d_pre_recv[...])
        tower_part[here, :] = total.astype(BF16)
    loop(0, nx, tower_rows)

    def send_x(k):
        to = lax.rem(x + k, nx)
        copy(8, tower_part.at[block(to, wide)], tower_x.at[x], at(z, to, core)).start()
    loop(1, nx, send_x)

    def squeeze(i):
        here = block(i, n)
        high, low = halves(nt(d_gates[here, :width], expand) + nt(d_gates[here, width:], expand))
        d_users[here, 2 * width:2 * width + LANES] = high
        d_users[here, 2 * width + LANES:] = low
    loop(0, 2 * QUARTERS, squeeze)

    tile_users = min(128, rows)

    def sum_users(t):
        index = iota((tile_users, n), 0) + t * tile_users
        put = jnp.concatenate(
            [ones_where(index == key_rows[side] + q) for side in range(2) for q in range(QUARTERS)], axis=1)
        total = nn(put, d_users[...])
        here = block(t, tile_users)
        users_part[here, :width] = total[:, :width] + total[:, width:2 * width]
        users_part[here, width:] = total[:, 2 * width:2 * width + LANES] + total[:, 2 * width + LANES:]
    loop(0, rows // tile_users, sum_users)
    theirs = pl.ds(pl.multiple_of((1 - core) * half, half), half)
    copy(7, users_part.at[theirs], users_part_recv, partner).start()
    wait_recv(7, users_part_recv)
    users_half[...] = (users_part[mine, :] + users_part_recv[...]).astype(BF16)
    tall = nz * BLOCK

    def send_ux(k):
        to = lax.rem(x + k, nx)
        copy(9, users_half.at[block(to, tall)], users_x.at[x], at(z, to, core)).start()
    loop(1, nx, send_ux)

    wait_recv(8, tower_x.at[pl.ds(0, nx - 1)])
    total = tower_part[block(x, wide), :].astype(F32)
    for k in range(1, nx):
        total = total + tower_x[lax.rem(x + k, nx)].astype(F32)
    tower_mid[...] = total.astype(BF16)

    def send_z(k):
        to = lax.rem(z + k, nz)
        copy(10, tower_mid.at[block(to, depth)], tower_z.at[z], at(to, x, core)).start()
    loop(1, nz, send_z)

    wait_recv(9, users_x.at[pl.ds(0, nx - 1)])
    total = users_half[block(x, tall), :].astype(F32)
    for k in range(1, nx):
        total = total + users_x[lax.rem(x + k, nx)].astype(F32)
    users_mid[...] = total.astype(BF16)

    def send_uz(k):
        to = lax.rem(z + k, nz)
        copy(11, users_mid.at[block(to, BLOCK)], users_z.at[z], at(to, x, core)).start()
    loop(1, nz, send_uz)

    wait_recv(6, back_recv.at[pl.ds(0, rows - BLOCK)])
    quarter_row = iota((1, rows), 1) & 3
    for q in range(QUARTERS):
        key = jnp.where(quarter_row == q, asked_row, -1)
        pick = ones_where(key == iota((slots, rows), 0))
        table_out[:, q * width:(q + 1) * width] = nn(pick, back_recv[...])

    wait_recv(10, tower_z.at[pl.ds(0, nz - 1)])
    total = tower_mid[block(z, depth), :].astype(F32)
    for k in range(1, nz):
        total = total + tower_z[lax.rem(z + k, nz)].astype(F32)
    tower_low[...] = total.astype(BF16)

    def send_y(k):
        copy(12, tower_low, tower_y.at[g], (lax.rem(g + k, groups), s)).start()
    loop(1, groups, send_y)

    wait_recv(11, users_z.at[pl.ds(0, nz - 1)])
    total = users_mid[block(z, BLOCK), :].astype(F32)
    for k in range(1, nz):
        total = total + users_z[lax.rem(z + k, nz)].astype(F32)
    users_out[...] = total[:, :width]
    gates_out[...] = total[:, width:]

    tower_y[g] = tower_low[...]
    wait_recv(12, tower_y.at[pl.ds(0, groups - 1)])
    total = tower_y[0].astype(F32)
    for k in range(1, groups):
        total = total + tower_y[k].astype(F32)
    tower_out[...] = total

    wait_send(0, head_send.at[pl.ds(0, shards - 1)])
    wait_send(1, users_all.at[others])
    wait_send(2, xt_recv)
    wait_send(3, rows_send.at[pl.ds(0, rows - BLOCK)])
    wait_send(4, users_all.at[mine])
    wait_send(5, d_pre)
    wait_send(6, back_send.at[pl.ds(0, rows - BLOCK)])
    wait_send(7, users_part_recv)
    wait_send(8, tower_x.at[pl.ds(0, nx - 1)])
    wait_send(9, users_x.at[pl.ds(0, nx - 1)])
    wait_send(10, tower_z.at[pl.ds(0, nz - 1)])
    wait_send(11, users_z.at[pl.ds(0, nz - 1)])
    wait_send(12, tower_y.at[pl.ds(0, groups - 1)])


def local(item_features, tower_weight, item_table, owner, table_slot, pair_users, user_comps, user_gates):
    groups, shards = lax.axis_size("group"), lax.axis_size("shard")
    nx = 4 if shards >= 64 else 2
    nz = shards // (nx * CORES)
    n, d = item_features.shape
    slots = item_table.shape[0]
    held = user_comps.shape[0]
    width = d // QUARTERS
    rows = shards * BLOCK
    half = rows // CORES
    depth = d // shards
    across = width + LANES
    ids = jnp.concatenate(
        [owner.reshape(1, n), table_slot.reshape(1, n), pair_users.T], axis=0)
    gates = user_gates.reshape(held * QUARTERS, -1)
    own_users = jnp.concatenate(
        [user_comps.reshape(BLOCK, width), jnp.pad(gates, ((0, 0), (0, LANES - gates.shape[1])))], axis=1)
    scratch = [
        ((shards, 1, LANES), F32), ((shards, 1, LANES), F32),
        ((rows, across), BF16),
        ((CORES, d // 2, n), BF16), ((d // 2, n), BF16),
        ((QUARTERS * n, width), BF16), ((n, d), F32),
        ((rows, width), BF16), ((rows, width), BF16),
        ((2 * QUARTERS * n, width), BF16), ((2 * QUARTERS * n, width), BF16),
        ((QUARTERS * n, width), F32), ((QUARTERS * n, width), BF16),
        ((n, d), BF16), ((n, d), BF16),
        ((2 * QUARTERS * n, 2 * across), BF16), ((2 * QUARTERS * n, 2 * width), BF16),
        ((rows, across), F32), ((half, across), F32),
        ((d // 2, d), BF16), ((nx, nz * depth, d), BF16), ((nz * depth, d), BF16),
        ((nz, depth, d), BF16), ((depth, d), BF16), ((groups, depth, d), BF16),
        ((half, across), BF16), ((nx, nz * BLOCK, across), BF16), ((nz * BLOCK, across), BF16),
        ((nz, BLOCK, across), BF16),
        ((rows, width), BF16), ((rows, width), BF16),
    ]
    whole = pl.BlockSpec(memory_space=pltpu.VMEM)
    tower_grad, table_grad, user_rows, gate_rows = pl.pallas_call(
        functools.partial(kernel, groups, shards, nx),
        out_shape=(
            jax.ShapeDtypeStruct((depth, d), F32),
            jax.ShapeDtypeStruct((slots, d), F32),
            jax.ShapeDtypeStruct((BLOCK, width), F32),
            jax.ShapeDtypeStruct((BLOCK, LANES), F32),
        ),
        in_specs=[whole] * 5,
        out_specs=(whole,) * 4,
        scratch_shapes=[pltpu.VMEM(shape, kind) for shape, kind in scratch]
        + [pltpu.SemaphoreType.DMA((13,)), pltpu.SemaphoreType.DMA((13,))],
        compiler_params=pltpu.CompilerParams(
            collective_id=0, has_side_effects=True, vmem_limit_bytes=56 * 1024 * 1024),
    )(ids, item_features, tower_weight, item_table, own_users)
    user_comp_grad = user_rows.reshape(held, d)
    user_gate_grad = gate_rows[:, : gates.shape[1]].reshape(held, -1)
    return tower_grad, table_grad, user_comp_grad, user_gate_grad


def solution(mesh):
    spread = P(("group", "shard"), None)
    return jax.shard_map(
        local,
        mesh=mesh,
        in_specs=(spread, P(), spread, spread, P(("group", "shard")), spread, spread, spread),
        out_specs=(P("shard", None), spread, spread, spread),
        check_vma=False,
    )
```

```python
import functools

import jax
import jax.numpy as jnp
from jax import lax
from jax.experimental import pallas as pl
from jax.experimental.pallas import tpu as pltpu
from jax.sharding import PartitionSpec as P

MESH = pl.DeviceIdType.MESH
COMPS = 8
CAP = 4
CORES = 2
QUARTERS = 4
BLOCK = CAP * QUARTERS
GROUP = 16
LANES = 128
F32, BF16 = jnp.float32, jnp.bfloat16


def nn(a, b):
    return lax.dot_general(a, b, (((1,), (0,)), ((), ())), preferred_element_type=F32)


def nt(a, b):
    return lax.dot_general(a, b, (((1,), (1,)), ((), ())), preferred_element_type=F32)


def tn(a, b):
    return lax.dot_general(a, b, (((0,), (0,)), ((), ())), preferred_element_type=F32)


def ones_where(condition):
    return jnp.where(condition, 1.0, 0.0).astype(BF16)


def iota(shape, dim):
    return lax.broadcasted_iota(jnp.int32, shape, dim)


def halves(values):
    high = values.astype(BF16)
    return high, (values - high.astype(F32)).astype(BF16)


def sigmoid(values):
    return 1.0 / (1.0 + jnp.exp(-values))


def kernel(
    groups, shards, nx,
    owner_ref, slot_ref, pair_ref, x_ref, w_hbm, table_ref, comps_ref, gates_ref,
    tower_out, table_out, users_out, gates_out,
    w_ref, own_rows, own_users, head_send, head_recv, users_all, xt, xt_recv, embedded, slope, rows_send, rows_recv,
    picked, gates_wide, combined, d_comb, d_pre, d_pre_recv, d_users, d_gates,
    users_part, users_part_recv, tower_part, tower_x, tower_mid, tower_z, tower_low, tower_y,
    users_half, users_x, users_mid, users_z, back_send, back_recv,
    send_sems, recv_sems, head_sems, w_sem,
):
    n, d = x_ref.shape
    slots = table_ref.shape[0]
    width = d // QUARTERS
    rows = shards * BLOCK
    half = rows // CORES
    nz = shards // (nx * CORES)
    depth = d // shards
    chips = shards // CORES
    g, s = lax.axis_index("group"), lax.axis_index("shard")
    core = lax.rem(s, CORES)
    chip = lax.div(s, CORES)
    x, z = lax.rem(chip, nx), lax.div(chip, nx)

    def at(z_to, x_to, core_to):
        return (g, (z_to * nx + x_to) * CORES + core_to)

    partner = at(z, x, 1 - core)

    def copy(number, source, target, device):
        return pltpu.make_async_remote_copy(
            src_ref=source, dst_ref=target,
            send_sem=send_sems.at[number], recv_sem=recv_sems.at[number],
            device_id=device, device_id_type=MESH,
        )

    def wait_recv(number, whole):
        copy(number, whole, whole, partner).wait_recv()

    def wait_send(number, whole):
        copy(number, whole, whole, partner).wait_send()

    def loop(low, high, step):
        def run(i, carry):
            step(i)
            return carry
        lax.fori_loop(low, high, run, 0)

    def block(i, size):
        return pl.ds(pl.multiple_of(i * size, size), size)

    load_w = pltpu.make_async_copy(w_hbm, w_ref, w_sem)
    load_w.start()
    barrier = pltpu.get_barrier_semaphore()
    loop(1, shards, lambda k: pl.semaphore_signal(
        barrier, inc=1, device_id=(g, lax.rem(s + k, shards)), device_id_type=MESH))
    loop(1, groups, lambda k: pl.semaphore_signal(
        barrier, inc=1, device_id=(lax.rem(g + k, groups), s), device_id_type=MESH))

    target = owner_ref[...]
    slot = slot_ref[...]
    to_owner = jnp.where(iota((shards, n), 0) == target, 1.0, 0.0)
    earlier = ones_where(iota((n, n), 0) < iota((n, n), 1))
    before = nn(to_owner.astype(BF16), earlier)
    within = jnp.sum(before * to_owner, axis=0, keepdims=True).astype(jnp.int32)
    place_row = (target * CAP + within) * QUARTERS
    eye = iota((n, n), 0) == iota((n, n), 1)

    def as_column(row):
        wide = jnp.where(eye, row.astype(F32), 0.0)
        return jnp.sum(wide, axis=1, keepdims=True).astype(jnp.int32)

    place_col = as_column(place_row)
    wanted = (to_owner * (slot + 1).astype(F32)).astype(BF16)
    turn = ones_where(iota((LANES, n), 0) == within)
    head_send[...] = nt(wanted, turn).reshape(shards, 1, LANES)

    own_rows[:, width:] = jnp.zeros((BLOCK, LANES), F32)
    gate_lane = iota((1, COMPS * COMPS), 1)
    own_comps, own_gates = comps_ref[...].astype(F32), gates_ref[...].astype(F32)
    for u in range(CAP):
        for q in range(QUARTERS):
            row = u * QUARTERS + q
            own_rows[row:row + 1, :width] = own_comps[u:u + 1, q * width:(q + 1) * width]
            own_rows[row:row + 1, width:width + COMPS * COMPS] = jnp.where(
                (gate_lane >> 4) == q, own_gates[u:u + 1, :], 0.0)
    own_users[...] = own_rows[...].astype(BF16)
    own = core * chips + x * nz + z
    users_all[block(own, BLOCK), :] = own_users[...]

    pl.semaphore_wait(barrier, shards - 1 + groups - 1)

    column = nx * CORES

    def head(away, p):
        return pltpu.make_async_remote_copy(
            src_ref=head_send.at[p], dst_ref=head_recv.at[s],
            send_sem=send_sems.at[0], recv_sem=head_sems.at[away],
            device_id=(g, p), device_id_type=MESH,
        )

    def send_head(k):
        p = lax.rem(s + k, shards)
        head(lax.rem(z - lax.div(p, column) + nz, nz), p).start()
    loop(1, shards, send_head)
    head_recv[s] = head_send[s]

    def send_users(k):
        p = lax.rem(chip + k, chips)
        copy(1, own_users, users_all.at[block(own, BLOCK)], (g, p * CORES + core)).start()
    loop(1, chips, send_users)
    for tile in range(d // LANES):
        turned = x_ref[:, tile * LANES:(tile + 1) * LANES].astype(F32).T.astype(BF16)
        for piece in range(max(1, LANES // depth)):
            size = min(depth, LANES)
            first = tile * LANES + piece * size
            holder, rest = divmod(first, depth)
            c_h, chip_h = holder % CORES, holder // CORES
            row = ((chip_h % nx) * nz + chip_h // nx) * depth + rest
            xt[c_h, row:row + size, :] = turned[piece * size:(piece + 1) * size]

    copy(2, xt.at[1 - core], xt_recv, partner).start()

    load_w.wait()

    def tower(q):
        columns = block(q, width)
        pre = nn(x_ref[...], w_ref[:, columns])
        share = 0.5 + 0.5 * lax.erf(pre * (0.5 ** 0.5))
        embedded[block(q, n), :] = (pre * share).astype(BF16)
        slope[:, columns] = share + pre * (0.3989422804014327 * jnp.exp(-0.5 * pre * pre))
    loop(0, QUARTERS, tower)

    tile_rows = min(256, rows)
    span = column * BLOCK

    def answer(step):
        away = (step + 1) >> 1
        off = jnp.where((step & 1) == 1, away, nz - away)
        z_from = lax.rem(z + off, nz)
        first = z_from * column

        @pl.when(step == 0)
        def _():
            pltpu.make_async_copy(
                head_recv.at[pl.ds(0, column - 1)], head_recv.at[pl.ds(0, column - 1)], head_sems.at[0]).wait()

        @pl.when(step > 0)
        def _():
            whole = head_recv.at[pl.ds(0, column)]
            pltpu.make_async_copy(whole, whole, head_sems.at[lax.rem(off, nz)]).wait()

        heads = head_recv[pl.ds(first, column)].reshape(column, LANES).astype(BF16)
        spread = nn(ones_where((iota((span, column), 0) >> 4) == iota((span, column), 1)), heads)
        index = iota((span, LANES), 0)
        mine = jnp.where(((index >> 2) & 3) == iota((span, LANES), 1), spread, 0.0)
        asked = jnp.sum(mine, axis=1, keepdims=True).astype(jnp.int32) - 1
        quarter = index[:, 0:1] & 3
        out = jnp.zeros((span, width), F32)
        for q in range(QUARTERS):
            key = jnp.where(quarter == q, asked, -1)
            pick = ones_where(key == iota((span, slots), 1))
            out = out + nn(pick, table_ref[:, q * width:(q + 1) * width])
        rows_send[block(z_from, span), :] = out.astype(BF16)

        def send_rows(k):
            p = first + k

            @pl.when(p != s)
            def _():
                copy(3, rows_send.at[block(p, BLOCK)], rows_recv.at[block(s, BLOCK)], (g, p)).start()
        loop(0, column, send_rows)
    loop(0, nz, answer)
    rows_recv[block(s, BLOCK), :] = rows_send[block(s, BLOCK), :]

    others = pl.ds(0, half - BLOCK)
    wait_recv(1, users_all.at[others])
    mine = pl.ds(pl.multiple_of(core * half, half), half)
    copy(4, users_all.at[mine], users_all.at[mine], partner).start()

    heads = head_recv[...].reshape(shards, LANES).astype(BF16)
    held = tn(heads, ones_where((iota((shards, rows), 1) >> 4) == iota((shards, rows), 0)))
    lane = iota((LANES, rows), 1)
    held = jnp.where(((lane >> 2) & 3) == iota((LANES, rows), 0), held, 0.0)
    asked_row = jnp.sum(held, axis=0, keepdims=True).astype(jnp.int32) - 1

    def user_key(row):
        user, holder = row & 3, row >> 2
        c_u, chip_u = holder & 1, holder >> 1
        where = c_u * chips + (chip_u & (nx - 1)) * nz + (chip_u >> (nx.bit_length() - 1))
        return (where * CAP + user) * QUARTERS

    key_rows = [user_key(pair_ref[side:side + 1, :]) for side in range(2)]
    key_cols = [as_column(row) for row in key_rows]
    gate = iota((LANES, width), 0)
    expand = ones_where((gate < COMPS * COMPS) & ((gate & 15) == (iota((LANES, width), 1) >> 4)))
    wait_recv(4, users_all.at[mine])
    for side in range(2):
        def pick_users(q):
            pick = ones_where(key_cols[side] + q == iota((n, rows), 1))
            got = nn(pick, users_all[...]).astype(BF16)
            here = block(side * QUARTERS + q, n)
            picked[here, :] = got[:, :width]
            gates_wide[here, :] = nn(got[:, width:], expand).astype(BF16)
        loop(0, QUARTERS, pick_users)

    wait_recv(3, rows_recv.at[pl.ds(0, rows - BLOCK)])

    def combine(q):
        pick = ones_where(place_col + q == iota((n, rows), 1))
        here = block(q, n)
        combined[here, :] = embedded[here, :].astype(F32) + nn(pick, rows_recv[...])
    loop(0, QUARTERS, combine)

    def spot(index, b):
        return pl.ds(pl.multiple_of(index * n + b * GROUP, GROUP), GROUP)

    def lanes_of(p):
        return slice((p & 1) * LANES, (p & 1) * LANES + LANES)

    def stack(ref, b, sides):
        return jnp.concatenate(
            [ref[spot(side * QUARTERS + (p >> 1), b), lanes_of(p)] for side in range(sides) for p in range(COMPS)],
            axis=0)

    pairs = COMPS * GROUP

    def pair_loss(b):
        stores = []

        def store(ref, where, lanes, values):
            stores.append((ref, where, lanes, values))

        comb = stack(combined, b, 1)
        scale = lax.rsqrt(jnp.mean(comb * comb, axis=1, keepdims=True) + 1e-06)
        normed = comb * scale
        n_high, n_low = halves(normed)
        users = stack(picked, b, 2)
        gates = stack(gates_wide, b, 2).astype(F32)
        logits = nt(users, n_high) + nt(users, n_low)
        same = (iota((2 * pairs, pairs), 0) & (GROUP - 1)) == (iota((2 * pairs, pairs), 1) & (GROUP - 1))
        weights = sigmoid(gates + logits)
        terms = jnp.where(same, weights * logits, 0.0)
        factors = []
        for side in range(2):
            total = terms[side * pairs:side * pairs + GROUP]
            for p in range(1, COMPS):
                total = total + terms[side * pairs + p * GROUP:side * pairs + (p + 1) * GROUP]
            score = 0.125 * jnp.sum(total, axis=1, keepdims=True)
            factor = sigmoid(score) if side else -sigmoid(-score)
            factors += [0.125 * factor] * COMPS
        factor = jnp.where(same, jnp.concatenate(factors, axis=0), 0.0)
        bend = logits * (weights * (1.0 - weights))
        dg_high, dg_low = halves(factor * bend)
        dl = factor * (weights + bend)
        dl_high, dl_low = halves(dl)
        d_normed = tn(dl_high, users) + tn(dl_low, users)
        du_high, du_low = halves(nn(dl_high, n_high) + nn(dl_low, n_high) + nn(dl_high, n_low))
        d_row = scale * (d_normed - normed * jnp.mean(d_normed * normed, axis=1, keepdims=True))
        d_row = d_row.astype(BF16)
        for p in range(COMPS):
            part = d_row[p * GROUP:(p + 1) * GROUP]
            store(d_comb, spot(p >> 1, b), lanes_of(p), part)
            item, column = block(b, GROUP), slice(p * LANES, (p + 1) * LANES)
            store(d_pre, item, column, (part.astype(F32) * slope[item, column]).astype(BF16))
        for side in range(2):
            for p in range(COMPS):
                here = spot(side * QUARTERS + (p >> 1), b)
                part = slice(side * pairs + p * GROUP, side * pairs + (p + 1) * GROUP)
                lane0 = (p & 1) * LANES
                store(d_users, here, slice(lane0, lane0 + LANES), du_high[part])
                store(d_users, here, slice(width + lane0, width + lane0 + LANES), du_low[part])
                store(d_gates, here, slice(lane0, lane0 + LANES), dg_high[part])
                store(d_gates, here, slice(width + lane0, width + lane0 + LANES), dg_low[part])
        return stores

    together = 2 - (n // GROUP) % 2

    def pair_losses(t):
        for stores in [pair_loss(t * together + i) for i in range(together)]:
            for ref, where, lanes, values in stores:
                ref[where, lanes] = values
    loop(0, n // (GROUP * together), pair_losses)

    copy(5, d_pre, d_pre_recv, partner).start()

    def give_back(t):
        index = iota((tile_rows, n), 0) + t * tile_rows
        put = jnp.concatenate([ones_where(index == place_row + q) for q in range(QUARTERS)], axis=1)
        back_send[block(t, tile_rows), :] = nn(put, d_comb[...]).astype(BF16)
    loop(0, rows // tile_rows, give_back)

    wait_recv(2, xt_recv)
    wait_recv(5, d_pre_recv)
    wide = nz * depth

    def tower_rows(i):
        here = block(i, wide)
        total = nn(xt[core, here, :], d_pre[...]) + nn(xt_recv[here, :], d_pre_recv[...])
        tower_part[here, :] = total.astype(BF16)
    loop(0, nx, tower_rows)

    def send_x(k):
        to = lax.rem(x + k, nx)
        copy(8, tower_part.at[block(to, wide)], tower_x.at[x], at(z, to, core)).start()
    loop(1, nx, send_x)

    def send_back(k):
        p = lax.rem(s + k, shards)
        copy(6, back_send.at[block(p, BLOCK)], back_recv.at[block(s, BLOCK)], (g, p)).start()
    loop(1, shards, send_back)
    back_recv[block(s, BLOCK), :] = back_send[block(s, BLOCK), :]

    def squeeze(i):
        here = block(i, n)
        high, low = halves(nt(d_gates[here, :width], expand) + nt(d_gates[here, width:], expand))
        ours = (iota((n, LANES), 1) >> 4) == (i & 3)
        zero = jnp.zeros((n, LANES), BF16)
        d_users[here, 2 * width:2 * width + LANES] = jnp.where(ours, high, zero)
        d_users[here, 2 * width + LANES:] = jnp.where(ours, low, zero)
    loop(0, 2 * QUARTERS, squeeze)

    tile_users = min(128, rows)

    def sum_users(t):
        index = iota((tile_users, n), 0) + t * tile_users
        put = jnp.concatenate(
            [ones_where(index == key_rows[side] + q) for side in range(2) for q in range(QUARTERS)], axis=1)
        total = nn(put, d_users[...])
        here = block(t, tile_users)
        users_part[here, :width] = total[:, :width] + total[:, width:2 * width]
        users_part[here, width:] = total[:, 2 * width:2 * width + LANES] + total[:, 2 * width + LANES:]
    loop(0, rows // tile_users, sum_users)
    theirs = pl.ds(pl.multiple_of((1 - core) * half, half), half)
    copy(7, users_part.at[theirs], users_part_recv, partner).start()
    wait_recv(7, users_part_recv)
    users_half[...] = (users_part[mine, :] + users_part_recv[...]).astype(BF16)
    tall = nz * BLOCK

    def send_ux(k):
        to = lax.rem(x + k, nx)
        copy(9, users_half.at[block(to, tall)], users_x.at[x], at(z, to, core)).start()
    loop(1, nx, send_ux)

    wait_recv(8, tower_x.at[pl.ds(0, nx - 1)])
    total = tower_part[block(x, wide), :].astype(F32)
    for k in range(1, nx):
        total = total + tower_x[lax.rem(x + k, nx)].astype(F32)
    tower_mid[...] = total.astype(BF16)

    def send_z(k):
        to = lax.rem(z + k, nz)
        copy(10, tower_mid.at[block(to, depth)], tower_z.at[z], at(to, x, core)).start()
    loop(1, nz, send_z)

    wait_recv(9, users_x.at[pl.ds(0, nx - 1)])
    total = users_half[block(x, tall), :].astype(F32)
    for k in range(1, nx):
        total = total + users_x[lax.rem(x + k, nx)].astype(F32)
    users_mid[...] = total.astype(BF16)

    def send_uz(k):
        to = lax.rem(z + k, nz)
        copy(11, users_mid.at[block(to, BLOCK)], users_z.at[z], at(to, x, core)).start()
    loop(1, nz, send_uz)

    wait_recv(6, back_recv.at[pl.ds(0, rows - BLOCK)])
    quarter_row = iota((1, rows), 1) & 3
    for q in range(QUARTERS):
        key = jnp.where(quarter_row == q, asked_row, -1)
        pick = ones_where(key == iota((slots, rows), 0))
        table_out[:, q * width:(q + 1) * width] = nn(pick, back_recv[...])

    wait_recv(10, tower_z.at[pl.ds(0, nz - 1)])
    total = tower_mid[block(z, depth), :].astype(F32)
    for k in range(1, nz):
        total = total + tower_z[lax.rem(z + k, nz)].astype(F32)
    tower_low[...] = total.astype(BF16)

    def send_y(k):
        copy(12, tower_low, tower_y.at[g], (lax.rem(g + k, groups), s)).start()
    loop(1, groups, send_y)

    wait_recv(11, users_z.at[pl.ds(0, nz - 1)])
    total = users_mid[block(z, BLOCK), :].astype(F32)
    for k in range(1, nz):
        total = total + users_z[lax.rem(z + k, nz)].astype(F32)
    own_rows[...] = total
    for u in range(CAP):
        gate_row = jnp.zeros((1, COMPS * COMPS), F32)
        for q in range(QUARTERS):
            row = u * QUARTERS + q
            users_out[u:u + 1, q * width:(q + 1) * width] = own_rows[row:row + 1, :width]
            gate_row = gate_row + own_rows[row:row + 1, width:width + COMPS * COMPS]
        gates_out[u:u + 1, :] = gate_row

    tower_y[g] = tower_low[...]
    wait_recv(12, tower_y.at[pl.ds(0, groups - 1)])
    total = tower_y[0].astype(F32)
    for k in range(1, groups):
        total = total + tower_y[k].astype(F32)
    tower_out[...] = total

    wait_send(0, head_send.at[pl.ds(0, shards - 1)])
    wait_send(1, users_all.at[others])
    wait_send(2, xt_recv)
    wait_send(3, rows_send.at[pl.ds(0, rows - BLOCK)])
    wait_send(4, users_all.at[mine])
    wait_send(5, d_pre)
    wait_send(6, back_send.at[pl.ds(0, rows - BLOCK)])
    wait_send(7, users_part_recv)
    wait_send(8, tower_x.at[pl.ds(0, nx - 1)])
    wait_send(9, users_x.at[pl.ds(0, nx - 1)])
    wait_send(10, tower_z.at[pl.ds(0, nz - 1)])
    wait_send(11, users_z.at[pl.ds(0, nz - 1)])
    wait_send(12, tower_y.at[pl.ds(0, groups - 1)])


def local(item_features, tower_weight, item_table, owner, table_slot, pair_users, user_comps, user_gates):
    groups, shards = lax.axis_size("group"), lax.axis_size("shard")
    nx = 4 if shards >= 64 else 2
    nz = shards // (nx * CORES)
    n, d = item_features.shape
    slots = item_table.shape[0]
    held = user_comps.shape[0]
    width = d // QUARTERS
    rows = shards * BLOCK
    half = rows // CORES
    depth = d // shards
    across = width + LANES
    scratch = [
        ((d, d), BF16), ((BLOCK, across), F32), ((BLOCK, across), BF16),
        ((shards, 1, LANES), F32), ((shards, 1, LANES), F32),
        ((rows, across), BF16),
        ((CORES, d // 2, n), BF16), ((d // 2, n), BF16),
        ((QUARTERS * n, width), BF16), ((n, d), F32),
        ((rows, width), BF16), ((rows, width), BF16),
        ((2 * QUARTERS * n, width), BF16), ((2 * QUARTERS * n, width), BF16),
        ((QUARTERS * n, width), F32), ((QUARTERS * n, width), BF16),
        ((n, d), BF16), ((n, d), BF16),
        ((2 * QUARTERS * n, 2 * across), BF16), ((2 * QUARTERS * n, 2 * width), BF16),
        ((rows, across), F32), ((half, across), F32),
        ((d // 2, d), BF16), ((nx, nz * depth, d), BF16), ((nz * depth, d), BF16),
        ((nz, depth, d), BF16), ((depth, d), BF16), ((groups, depth, d), BF16),
        ((half, across), BF16), ((nx, nz * BLOCK, across), BF16), ((nz * BLOCK, across), BF16),
        ((nz, BLOCK, across), BF16),
        ((rows, width), BF16), ((rows, width), BF16),
    ]
    whole = pl.BlockSpec(memory_space=pltpu.VMEM)
    return pl.pallas_call(
        functools.partial(kernel, groups, shards, nx),
        out_shape=(
            jax.ShapeDtypeStruct((depth, d), F32),
            jax.ShapeDtypeStruct((slots, d), F32),
            jax.ShapeDtypeStruct((held, d), F32),
            jax.ShapeDtypeStruct((held, COMPS * COMPS), F32),
        ),
        in_specs=[whole] * 4 + [pl.BlockSpec(memory_space=pltpu.HBM)] + [whole] * 3,
        out_specs=(whole,) * 4,
        scratch_shapes=[pltpu.VMEM(shape, kind) for shape, kind in scratch]
        + [pltpu.SemaphoreType.DMA((13,)), pltpu.SemaphoreType.DMA((13,)), pltpu.SemaphoreType.DMA((nz,)),
           pltpu.SemaphoreType.DMA],
        compiler_params=pltpu.CompilerParams(
            collective_id=0, has_side_effects=True, vmem_limit_bytes=32 * 1024 * 1024),
    )(owner.reshape(1, n), table_slot.reshape(1, n), pair_users.T, item_features, tower_weight, item_table,
      user_comps, user_gates)


def solution(mesh):
    spread = P(("group", "shard"), None)
    return jax.shard_map(
        local,
        mesh=mesh,
        in_specs=(spread, P(), spread, spread, P(("group", "shard")), spread, spread, spread),
        out_specs=(P("shard", None), spread, spread, spread),
        check_vma=False,
    )
```

```python
import functools

import jax
import jax.numpy as jnp
from jax import lax
from jax.experimental import pallas as pl
from jax.experimental.pallas import tpu as pltpu
from jax.sharding import PartitionSpec as P

MESH = pl.DeviceIdType.MESH
COMPS = 8
CAP = 4
CORES = 2
QUARTERS = 4
BLOCK = CAP * QUARTERS
GROUP = 16
LANES = 128
F32, BF16 = jnp.float32, jnp.bfloat16


def nn(a, b):
    return lax.dot_general(a, b, (((1,), (0,)), ((), ())), preferred_element_type=F32)


def nt(a, b):
    return lax.dot_general(a, b, (((1,), (1,)), ((), ())), preferred_element_type=F32)


def tn(a, b):
    return lax.dot_general(a, b, (((0,), (0,)), ((), ())), preferred_element_type=F32)


def ones_where(condition):
    return jnp.where(condition, 1.0, 0.0).astype(BF16)


def iota(shape, dim):
    return lax.broadcasted_iota(jnp.int32, shape, dim)


def halves(values):
    high = values.astype(BF16)
    return high, (values - high.astype(F32)).astype(BF16)


def sigmoid(values):
    return 1.0 / (1.0 + jnp.exp(-values))


def kernel(
    groups, shards, nx,
    owner_ref, slot_ref, pair_ref, x_ref, w_hbm, table_ref, comps_ref, gates_ref,
    tower_out, table_out, users_out, gates_out,
    w_ref, own_rows, own_users, head_send, head_recv, users_all, xt, xt_recv, embedded, slope, rows_send, rows_recv,
    picked, gates_wide, combined, d_comb, d_pre, d_pre_recv, d_users, d_gates,
    users_part, users_part_recv, tower_part, tower_x, tower_mid, tower_z, tower_low, tower_y,
    other_part, other_y, other_mid, other_x, other_low, other_z, other_got,
    users_half, users_x, users_mid, users_z, back_send, back_recv,
    send_sems, recv_sems, head_sems, w_sem,
):
    n, d = x_ref.shape
    slots = table_ref.shape[0]
    width = d // QUARTERS
    rows = shards * BLOCK
    half = rows // CORES
    nz = shards // (nx * CORES)
    depth = d // shards
    chips = shards // CORES
    g, s = lax.axis_index("group"), lax.axis_index("shard")
    core = lax.rem(s, CORES)
    chip = lax.div(s, CORES)
    x, z = lax.rem(chip, nx), lax.div(chip, nx)

    def at(z_to, x_to, core_to):
        return (g, (z_to * nx + x_to) * CORES + core_to)

    partner = at(z, x, 1 - core)

    def copy(number, source, target, device):
        return pltpu.make_async_remote_copy(
            src_ref=source, dst_ref=target,
            send_sem=send_sems.at[number], recv_sem=recv_sems.at[number],
            device_id=device, device_id_type=MESH,
        )

    def wait_recv(number, whole):
        copy(number, whole, whole, partner).wait_recv()

    def wait_send(number, whole):
        copy(number, whole, whole, partner).wait_send()

    def loop(low, high, step):
        def run(i, carry):
            step(i)
            return carry
        lax.fori_loop(low, high, run, 0)

    def block(i, size):
        return pl.ds(pl.multiple_of(i * size, size), size)

    load_w = pltpu.make_async_copy(w_hbm, w_ref, w_sem)
    load_w.start()
    barrier = pltpu.get_barrier_semaphore()
    loop(1, shards, lambda k: pl.semaphore_signal(
        barrier, inc=1, device_id=(g, lax.rem(s + k, shards)), device_id_type=MESH))
    loop(1, groups, lambda k: pl.semaphore_signal(
        barrier, inc=1, device_id=(lax.rem(g + k, groups), s), device_id_type=MESH))

    target = owner_ref[...]
    slot = slot_ref[...]
    to_owner = jnp.where(iota((shards, n), 0) == target, 1.0, 0.0)
    earlier = ones_where(iota((n, n), 0) < iota((n, n), 1))
    before = nn(to_owner.astype(BF16), earlier)
    within = jnp.sum(before * to_owner, axis=0, keepdims=True).astype(jnp.int32)
    place_row = (target * CAP + within) * QUARTERS
    eye = iota((n, n), 0) == iota((n, n), 1)

    def as_column(row):
        wide = jnp.where(eye, row.astype(F32), 0.0)
        return jnp.sum(wide, axis=1, keepdims=True).astype(jnp.int32)

    place_col = as_column(place_row)
    wanted = (to_owner * (slot + 1).astype(F32)).astype(BF16)
    turn = ones_where(iota((LANES, n), 0) == within)
    head_send[...] = nt(wanted, turn).reshape(shards, 1, LANES)

    own_rows[:, width:] = jnp.zeros((BLOCK, LANES), F32)
    gate_lane = iota((1, COMPS * COMPS), 1)
    own_comps, own_gates = comps_ref[...].astype(F32), gates_ref[...].astype(F32)
    for u in range(CAP):
        for q in range(QUARTERS):
            row = u * QUARTERS + q
            own_rows[row:row + 1, :width] = own_comps[u:u + 1, q * width:(q + 1) * width]
            own_rows[row:row + 1, width:width + COMPS * COMPS] = jnp.where(
                (gate_lane >> 4) == q, own_gates[u:u + 1, :], 0.0)
    own_users[...] = own_rows[...].astype(BF16)
    own = core * chips + x * nz + z
    users_all[block(own, BLOCK), :] = own_users[...]

    pl.semaphore_wait(barrier, shards - 1 + groups - 1)

    column = nx * CORES

    def head(away, p):
        return pltpu.make_async_remote_copy(
            src_ref=head_send.at[p], dst_ref=head_recv.at[s],
            send_sem=send_sems.at[0], recv_sem=head_sems.at[away],
            device_id=(g, p), device_id_type=MESH,
        )

    def send_head(k):
        p = lax.rem(s + k, shards)
        head(lax.rem(z - lax.div(p, column) + nz, nz), p).start()
    loop(1, shards, send_head)
    head_recv[s] = head_send[s]

    def send_users(k):
        p = lax.rem(chip + k, chips)
        copy(1, own_users, users_all.at[block(own, BLOCK)], (g, p * CORES + core)).start()
    loop(1, chips, send_users)
    for tile in range(d // LANES):
        turned = x_ref[:, tile * LANES:(tile + 1) * LANES].astype(F32).T.astype(BF16)
        for piece in range(max(1, LANES // depth)):
            size = min(depth, LANES)
            first = tile * LANES + piece * size
            holder, rest = divmod(first, depth)
            c_h, chip_h = holder % CORES, holder // CORES
            row = ((chip_h % nx) * nz + chip_h // nx) * depth + rest
            xt[c_h, row:row + size, :] = turned[piece * size:(piece + 1) * size]

    copy(2, xt.at[1 - core], xt_recv, partner).start()

    load_w.wait()

    def tower(q):
        columns = block(q, width)
        pre = nn(x_ref[...], w_ref[:, columns])
        share = 0.5 + 0.5 * lax.erf(pre * (0.5 ** 0.5))
        embedded[block(q, n), :] = (pre * share).astype(BF16)
        slope[:, columns] = share + pre * (0.3989422804014327 * jnp.exp(-0.5 * pre * pre))
    loop(0, QUARTERS, tower)

    tile_rows = min(256, rows)
    span = column * BLOCK

    def answer(step):
        away = (step + 1) >> 1
        off = jnp.where((step & 1) == 1, away, nz - away)
        z_from = lax.rem(z + off, nz)
        first = z_from * column

        @pl.when(step == 0)
        def _():
            pltpu.make_async_copy(
                head_recv.at[pl.ds(0, column - 1)], head_recv.at[pl.ds(0, column - 1)], head_sems.at[0]).wait()

        @pl.when(step > 0)
        def _():
            whole = head_recv.at[pl.ds(0, column)]
            pltpu.make_async_copy(whole, whole, head_sems.at[lax.rem(off, nz)]).wait()

        heads = head_recv[pl.ds(first, column)].reshape(column, LANES).astype(BF16)
        spread = nn(ones_where((iota((span, column), 0) >> 4) == iota((span, column), 1)), heads)
        index = iota((span, LANES), 0)
        mine = jnp.where(((index >> 2) & 3) == iota((span, LANES), 1), spread, 0.0)
        asked = jnp.sum(mine, axis=1, keepdims=True).astype(jnp.int32) - 1
        quarter = index[:, 0:1] & 3
        out = jnp.zeros((span, width), F32)
        for q in range(QUARTERS):
            key = jnp.where(quarter == q, asked, -1)
            pick = ones_where(key == iota((span, slots), 1))
            out = out + nn(pick, table_ref[:, q * width:(q + 1) * width])
        rows_send[block(z_from, span), :] = out.astype(BF16)

        def send_rows(k):
            p = first + k

            @pl.when(p != s)
            def _():
                copy(3, rows_send.at[block(p, BLOCK)], rows_recv.at[block(s, BLOCK)], (g, p)).start()
        loop(0, column, send_rows)
    loop(0, nz, answer)
    rows_recv[block(s, BLOCK), :] = rows_send[block(s, BLOCK), :]

    others = pl.ds(0, half - BLOCK)
    wait_recv(1, users_all.at[others])
    mine = pl.ds(pl.multiple_of(core * half, half), half)
    copy(4, users_all.at[mine], users_all.at[mine], partner).start()

    heads = head_recv[...].reshape(shards, LANES).astype(BF16)
    held = tn(heads, ones_where((iota((shards, rows), 1) >> 4) == iota((shards, rows), 0)))
    lane = iota((LANES, rows), 1)
    held = jnp.where(((lane >> 2) & 3) == iota((LANES, rows), 0), held, 0.0)
    asked_row = jnp.sum(held, axis=0, keepdims=True).astype(jnp.int32) - 1

    def user_key(row):
        user, holder = row & 3, row >> 2
        c_u, chip_u = holder & 1, holder >> 1
        where = c_u * chips + (chip_u & (nx - 1)) * nz + (chip_u >> (nx.bit_length() - 1))
        return (where * CAP + user) * QUARTERS

    key_rows = [user_key(pair_ref[side:side + 1, :]) for side in range(2)]
    key_cols = [as_column(row) for row in key_rows]
    gate = iota((LANES, width), 0)
    expand = ones_where((gate < COMPS * COMPS) & ((gate & 15) == (iota((LANES, width), 1) >> 4)))
    wait_recv(4, users_all.at[mine])
    for side in range(2):
        def pick_users(q):
            pick = ones_where(key_cols[side] + q == iota((n, rows), 1))
            got = nn(pick, users_all[...]).astype(BF16)
            here = block(side * QUARTERS + q, n)
            picked[here, :] = got[:, :width]
            gates_wide[here, :] = nn(got[:, width:], expand).astype(BF16)
        loop(0, QUARTERS, pick_users)

    wait_recv(3, rows_recv.at[pl.ds(0, rows - BLOCK)])

    def combine(q):
        pick = ones_where(place_col + q == iota((n, rows), 1))
        here = block(q, n)
        combined[here, :] = embedded[here, :].astype(F32) + nn(pick, rows_recv[...])
    loop(0, QUARTERS, combine)

    def spot(index, b):
        return pl.ds(pl.multiple_of(index * n + b * GROUP, GROUP), GROUP)

    def lanes_of(p):
        return slice((p & 1) * LANES, (p & 1) * LANES + LANES)

    def stack(ref, b, sides):
        return jnp.concatenate(
            [ref[spot(side * QUARTERS + (p >> 1), b), lanes_of(p)] for side in range(sides) for p in range(COMPS)],
            axis=0)

    pairs = COMPS * GROUP

    def pair_loss(b):
        stores = []

        def store(ref, where, lanes, values):
            stores.append((ref, where, lanes, values))

        comb = stack(combined, b, 1)
        scale = lax.rsqrt(jnp.mean(comb * comb, axis=1, keepdims=True) + 1e-06)
        normed = comb * scale
        n_high, n_low = halves(normed)
        users = stack(picked, b, 2)
        gates = stack(gates_wide, b, 2).astype(F32)
        logits = nt(users, n_high) + nt(users, n_low)
        same = (iota((2 * pairs, pairs), 0) & (GROUP - 1)) == (iota((2 * pairs, pairs), 1) & (GROUP - 1))
        weights = sigmoid(gates + logits)
        terms = jnp.where(same, weights * logits, 0.0)
        factors = []
        for side in range(2):
            total = terms[side * pairs:side * pairs + GROUP]
            for p in range(1, COMPS):
                total = total + terms[side * pairs + p * GROUP:side * pairs + (p + 1) * GROUP]
            score = 0.125 * jnp.sum(total, axis=1, keepdims=True)
            factor = sigmoid(score) if side else -sigmoid(-score)
            factors += [0.125 * factor] * COMPS
        factor = jnp.where(same, jnp.concatenate(factors, axis=0), 0.0)
        bend = logits * (weights * (1.0 - weights))
        dg_high, dg_low = halves(factor * bend)
        dl = factor * (weights + bend)
        dl_high, dl_low = halves(dl)
        d_normed = tn(dl_high, users) + tn(dl_low, users)
        du_high, du_low = halves(nn(dl_high, n_high) + nn(dl_low, n_high) + nn(dl_high, n_low))
        d_row = scale * (d_normed - normed * jnp.mean(d_normed * normed, axis=1, keepdims=True))
        d_row = d_row.astype(BF16)
        for p in range(COMPS):
            part = d_row[p * GROUP:(p + 1) * GROUP]
            store(d_comb, spot(p >> 1, b), lanes_of(p), part)
            item, column = block(b, GROUP), slice(p * LANES, (p + 1) * LANES)
            store(d_pre, item, column, (part.astype(F32) * slope[item, column]).astype(BF16))
        for side in range(2):
            for p in range(COMPS):
                here = spot(side * QUARTERS + (p >> 1), b)
                part = slice(side * pairs + p * GROUP, side * pairs + (p + 1) * GROUP)
                lane0 = (p & 1) * LANES
                store(d_users, here, slice(lane0, lane0 + LANES), du_high[part])
                store(d_users, here, slice(width + lane0, width + lane0 + LANES), du_low[part])
                store(d_gates, here, slice(lane0, lane0 + LANES), dg_high[part])
                store(d_gates, here, slice(width + lane0, width + lane0 + LANES), dg_low[part])
        return stores

    together = 2 - (n // GROUP) % 2

    def pair_losses(t):
        for stores in [pair_loss(t * together + i) for i in range(together)]:
            for ref, where, lanes, values in stores:
                ref[where, lanes] = values
    loop(0, n // (GROUP * together), pair_losses)

    copy(5, d_pre, d_pre_recv, partner).start()

    def give_back(t):
        index = iota((tile_rows, n), 0) + t * tile_rows
        put = jnp.concatenate([ones_where(index == place_row + q) for q in range(QUARTERS)], axis=1)
        back_send[block(t, tile_rows), :] = nn(put, d_comb[...]).astype(BF16)
    loop(0, rows // tile_rows, give_back)

    first = tower_part.shape[1]
    deep = nx * depth
    wait_recv(2, xt_recv)
    wait_recv(5, d_pre_recv)
    wide = nz * depth

    def tower_rows(i):
        here = block(i, wide)
        total = nn(xt[core, here, :], d_pre[...]) + nn(xt_recv[here, :], d_pre_recv[...])
        tower_part[here, :] = total[:, :first].astype(BF16)
        for j in range(nz):
            there = pl.ds(pl.multiple_of((j * nx + i) * depth, depth), depth)
            other_part[there, :] = total[j * depth:(j + 1) * depth, first:].astype(BF16)
    loop(0, nx, tower_rows)

    def send_x(k):
        to = lax.rem(x + k, nx)
        copy(8, tower_part.at[block(to, wide)], tower_x.at[x], at(z, to, core)).start()
    loop(1, nx, send_x)

    def send_other_y(k):
        to = lax.rem(g + k, groups)
        copy(13, other_part.at[block(to, deep)], other_y.at[g], (to, s)).start()
    loop(1, groups, send_other_y)

    def send_back(k):
        p = lax.rem(s + k, shards)
        copy(6, back_send.at[block(p, BLOCK)], back_recv.at[block(s, BLOCK)], (g, p)).start()
    loop(1, shards, send_back)
    back_recv[block(s, BLOCK), :] = back_send[block(s, BLOCK), :]

    def squeeze(i):
        here = block(i, n)
        high, low = halves(nt(d_gates[here, :width], expand) + nt(d_gates[here, width:], expand))
        ours = (iota((n, LANES), 1) >> 4) == (i & 3)
        zero = jnp.zeros((n, LANES), BF16)
        d_users[here, 2 * width:2 * width + LANES] = jnp.where(ours, high, zero)
        d_users[here, 2 * width + LANES:] = jnp.where(ours, low, zero)
    loop(0, 2 * QUARTERS, squeeze)

    tile_users = min(128, rows)

    def sum_users(t):
        index = iota((tile_users, n), 0) + t * tile_users
        put = jnp.concatenate(
            [ones_where(index == key_rows[side] + q) for side in range(2) for q in range(QUARTERS)], axis=1)
        total = nn(put, d_users[...])
        here = block(t, tile_users)
        users_part[here, :width] = total[:, :width] + total[:, width:2 * width]
        users_part[here, width:] = total[:, 2 * width:2 * width + LANES] + total[:, 2 * width + LANES:]
    loop(0, rows // tile_users, sum_users)
    theirs = pl.ds(pl.multiple_of((1 - core) * half, half), half)
    copy(7, users_part.at[theirs], users_part_recv, partner).start()
    wait_recv(7, users_part_recv)
    users_half[...] = (users_part[mine, :] + users_part_recv[...]).astype(BF16)
    tall = nz * BLOCK

    def send_ux(k):
        to = lax.rem(x + k, nx)
        copy(9, users_half.at[block(to, tall)], users_x.at[x], at(z, to, core)).start()
    loop(1, nx, send_ux)

    wait_recv(8, tower_x.at[pl.ds(0, nx - 1)])
    total = tower_part[block(x, wide), :].astype(F32)
    for k in range(1, nx):
        total = total + tower_x[lax.rem(x + k, nx)].astype(F32)
    tower_mid[...] = total.astype(BF16)

    def send_z(k):
        to = lax.rem(z + k, nz)
        copy(10, tower_mid.at[block(to, depth)], tower_z.at[z], at(to, x, core)).start()
    loop(1, nz, send_z)

    wait_recv(13, other_y.at[pl.ds(0, groups - 1)])
    total = other_part[block(g, deep), :].astype(F32)
    for k in range(1, groups):
        total = total + other_y[lax.rem(g + k, groups)].astype(F32)
    other_mid[...] = total.astype(BF16)

    def send_other_x(k):
        to = lax.rem(x + k, nx)
        copy(14, other_mid.at[block(to, depth)], other_x.at[x], at(z, to, core)).start()
    loop(1, nx, send_other_x)

    wait_recv(9, users_x.at[pl.ds(0, nx - 1)])
    total = users_half[block(x, tall), :].astype(F32)
    for k in range(1, nx):
        total = total + users_x[lax.rem(x + k, nx)].astype(F32)
    users_mid[...] = total.astype(BF16)

    def send_uz(k):
        to = lax.rem(z + k, nz)
        copy(11, users_mid.at[block(to, BLOCK)], users_z.at[z], at(to, x, core)).start()
    loop(1, nz, send_uz)

    wait_recv(14, other_x.at[pl.ds(0, nx - 1)])
    total = other_mid[block(x, depth), :].astype(F32)
    for k in range(1, nx):
        total = total + other_x[lax.rem(x + k, nx)].astype(F32)
    other_low[...] = total

    @pl.when(z != g)
    def _():
        copy(15, other_low, other_z.at[z], at(g, x, core)).start()

    wait_recv(10, tower_z.at[pl.ds(0, nz - 1)])
    total = tower_mid[block(z, depth), :].astype(F32)
    for k in range(1, nz):
        total = total + tower_z[lax.rem(z + k, nz)].astype(F32)
    tower_low[...] = total.astype(BF16)

    def send_y(k):
        copy(12, tower_low, tower_y.at[g], (lax.rem(g + k, groups), s)).start()
    loop(1, groups, send_y)

    @pl.when(z == g)
    def _():
        wait_recv(15, other_z.at[pl.ds(0, nz - 1)])
        total = other_low[...]
        for k in range(1, nz):
            total = total + other_z[lax.rem(z + k, nz)]
        other_got[...] = total.astype(BF16)

        def send_other(k):
            copy(16, other_got, other_got, (lax.rem(g + k, groups), s)).start()
        loop(1, groups, send_other)

    wait_recv(6, back_recv.at[pl.ds(0, rows - BLOCK)])
    quarter_row = iota((1, rows), 1) & 3
    for q in range(QUARTERS):
        key = jnp.where(quarter_row == q, asked_row, -1)
        pick = ones_where(key == iota((slots, rows), 0))
        table_out[:, q * width:(q + 1) * width] = nn(pick, back_recv[...])

    wait_recv(11, users_z.at[pl.ds(0, nz - 1)])
    total = users_mid[block(z, BLOCK), :].astype(F32)
    for k in range(1, nz):
        total = total + users_z[lax.rem(z + k, nz)].astype(F32)
    own_rows[...] = total
    for u in range(CAP):
        gate_row = jnp.zeros((1, COMPS * COMPS), F32)
        for q in range(QUARTERS):
            row = u * QUARTERS + q
            users_out[u:u + 1, q * width:(q + 1) * width] = own_rows[row:row + 1, :width]
            gate_row = gate_row + own_rows[row:row + 1, width:width + COMPS * COMPS]
        gates_out[u:u + 1, :] = gate_row

    tower_y[g] = tower_low[...]
    wait_recv(12, tower_y.at[pl.ds(0, groups - 1)])
    total = tower_y[0].astype(F32)
    for k in range(1, groups):
        total = total + tower_y[k].astype(F32)
    tower_out[:, :first] = total

    @pl.when(z != g)
    def _():
        wait_recv(16, other_got)
        wait_send(15, other_low)

    @pl.when(z == g)
    def _():
        wait_send(16, other_part.at[pl.ds(0, (groups - 1) * depth)])

    tower_out[:, first:] = other_got[...].astype(F32)
    wait_send(13, other_y.at[pl.ds(0, groups - 1)])
    wait_send(14, other_x.at[pl.ds(0, nx - 1)])

    wait_send(0, head_send.at[pl.ds(0, shards - 1)])
    wait_send(1, users_all.at[others])
    wait_send(2, xt_recv)
    wait_send(3, rows_send.at[pl.ds(0, rows - BLOCK)])
    wait_send(4, users_all.at[mine])
    wait_send(5, d_pre)
    wait_send(6, back_send.at[pl.ds(0, rows - BLOCK)])
    wait_send(7, users_part_recv)
    wait_send(8, tower_x.at[pl.ds(0, nx - 1)])
    wait_send(9, users_x.at[pl.ds(0, nx - 1)])
    wait_send(10, tower_z.at[pl.ds(0, nz - 1)])
    wait_send(11, users_z.at[pl.ds(0, nz - 1)])
    wait_send(12, tower_y.at[pl.ds(0, groups - 1)])


def local(item_features, tower_weight, item_table, owner, table_slot, pair_users, user_comps, user_gates):
    groups, shards = lax.axis_size("group"), lax.axis_size("shard")
    nx = 4 if shards >= 64 else 2
    nz = shards // (nx * CORES)
    n, d = item_features.shape
    slots = item_table.shape[0]
    held = user_comps.shape[0]
    width = d // QUARTERS
    rows = shards * BLOCK
    half = rows // CORES
    depth = d // shards
    across = width + LANES
    first = d * 5 // 8
    other = d - first
    assert groups == nz
    scratch = [
        ((d, d), BF16), ((BLOCK, across), F32), ((BLOCK, across), BF16),
        ((shards, 1, LANES), F32), ((shards, 1, LANES), F32),
        ((rows, across), BF16),
        ((CORES, d // 2, n), BF16), ((d // 2, n), BF16),
        ((QUARTERS * n, width), BF16), ((n, d), F32),
        ((rows, width), BF16), ((rows, width), BF16),
        ((2 * QUARTERS * n, width), BF16), ((2 * QUARTERS * n, width), BF16),
        ((QUARTERS * n, width), F32), ((QUARTERS * n, width), BF16),
        ((n, d), BF16), ((n, d), BF16),
        ((2 * QUARTERS * n, 2 * across), BF16), ((2 * QUARTERS * n, 2 * width), BF16),
        ((rows, across), F32), ((half, across), F32),
        ((d // 2, first), BF16), ((nx, nz * depth, first), BF16), ((nz * depth, first), BF16),
        ((nz, depth, first), BF16), ((depth, first), BF16), ((groups, depth, first), BF16),
        ((d // 2, other), BF16), ((groups, nx * depth, other), BF16), ((nx * depth, other), BF16),
        ((nx, depth, other), BF16), ((depth, other), F32), ((nz, depth, other), F32), ((depth, other), BF16),
        ((half, across), BF16), ((nx, nz * BLOCK, across), BF16), ((nz * BLOCK, across), BF16),
        ((nz, BLOCK, across), BF16),
        ((rows, width), BF16), ((rows, width), BF16),
    ]
    whole = pl.BlockSpec(memory_space=pltpu.VMEM)
    return pl.pallas_call(
        functools.partial(kernel, groups, shards, nx),
        out_shape=(
            jax.ShapeDtypeStruct((depth, d), F32),
            jax.ShapeDtypeStruct((slots, d), F32),
            jax.ShapeDtypeStruct((held, d), F32),
            jax.ShapeDtypeStruct((held, COMPS * COMPS), F32),
        ),
        in_specs=[whole] * 4 + [pl.BlockSpec(memory_space=pltpu.HBM)] + [whole] * 3,
        out_specs=(whole,) * 4,
        scratch_shapes=[pltpu.VMEM(shape, kind) for shape, kind in scratch]
        + [pltpu.SemaphoreType.DMA((17,)), pltpu.SemaphoreType.DMA((17,)), pltpu.SemaphoreType.DMA((nz,)),
           pltpu.SemaphoreType.DMA],
        compiler_params=pltpu.CompilerParams(
            collective_id=0, has_side_effects=True, vmem_limit_bytes=32 * 1024 * 1024),
    )(*(pltpu.with_memory_space_constraint(a, pltpu.HBM) for a in (
        owner.reshape(1, n), table_slot.reshape(1, n), pair_users.T, item_features, tower_weight, item_table,
        user_comps, user_gates)))


def solution(mesh):
    spread = P(("group", "shard"), None)
    return jax.shard_map(
        local,
        mesh=mesh,
        in_specs=(spread, P(), spread, spread, P(("group", "shard")), spread, spread, spread),
        out_specs=(P("shard", None), spread, spread, spread),
        check_vma=False,
    )
```

```python
import functools

import jax
import jax.numpy as jnp
from jax import lax
from jax.experimental import pallas as pl
from jax.experimental.pallas import tpu as pltpu
from jax.sharding import PartitionSpec as P

MESH = pl.DeviceIdType.MESH
COMPS = 8
CAP = 4
CORES = 2
QUARTERS = 4
BLOCK = CAP * QUARTERS
GROUP = 16
LANES = 128
F32, BF16 = jnp.float32, jnp.bfloat16


def nn(a, b):
    return lax.dot_general(a, b, (((1,), (0,)), ((), ())), preferred_element_type=F32)


def nt(a, b):
    return lax.dot_general(a, b, (((1,), (1,)), ((), ())), preferred_element_type=F32)


def tn(a, b):
    return lax.dot_general(a, b, (((0,), (0,)), ((), ())), preferred_element_type=F32)


def ones_where(condition):
    return jnp.where(condition, 1.0, 0.0).astype(BF16)


def iota(shape, dim):
    return lax.broadcasted_iota(jnp.int32, shape, dim)


def halves(values):
    high = values.astype(BF16)
    return high, (values - high.astype(F32)).astype(BF16)


def sigmoid(values):
    return 1.0 / (1.0 + jnp.exp(-values))


def kernel(
    groups, shards, nx,
    owner_hbm, slot_hbm, pair_hbm, comps_hbm, gates_hbm, x_hbm, w_hbm, table_hbm,
    tower_out, table_out, users_out, gates_out,
    owner_ref, slot_ref, pair_ref, comps_ref, gates_ref, x_ref, w_ref, table_ref,
    own_rows, own_users, own_gates, gates_all, head_send, head_recv, users_all, xt, xt_recv, embedded, slope, rows_send, rows_recv,
    picked, gates_wide, combined, d_comb, d_pre, d_pre_recv, d_users, d_gates,
    users_part, users_part_recv, tower_part, tower_x, tower_mid, tower_z, tower_low, tower_y,
    other_part, other_y, other_mid, other_x, other_low, other_z, other_got,
    users_half, users_x, users_mid, users_z, back_send, back_recv,
    send_sems, recv_sems, head_sems, load_sems,
):
    n, d = x_ref.shape
    slots = table_ref.shape[0]
    width = d // QUARTERS
    rows = shards * BLOCK
    half = rows // CORES
    nz = shards // (nx * CORES)
    depth = d // shards
    chips = shards // CORES
    g, s = lax.axis_index("group"), lax.axis_index("shard")
    core = lax.rem(s, CORES)
    chip = lax.div(s, CORES)
    x, z = lax.rem(chip, nx), lax.div(chip, nx)

    def at(z_to, x_to, core_to):
        return (g, (z_to * nx + x_to) * CORES + core_to)

    partner = at(z, x, 1 - core)

    def copy(number, source, target, device):
        return pltpu.make_async_remote_copy(
            src_ref=source, dst_ref=target,
            send_sem=send_sems.at[number], recv_sem=recv_sems.at[number],
            device_id=device, device_id_type=MESH,
        )

    def wait_recv(number, whole):
        copy(number, whole, whole, partner).wait_recv()

    def wait_send(number, whole):
        copy(number, whole, whole, partner).wait_send()

    def loop(low, high, step):
        def run(i, carry):
            step(i)
            return carry
        lax.fori_loop(low, high, run, 0)

    def block(i, size):
        return pl.ds(pl.multiple_of(i * size, size), size)

    loads = [
        pltpu.make_async_copy(source, target, load_sems.at[i])
        for i, (source, target) in enumerate((
            (owner_hbm, owner_ref), (slot_hbm, slot_ref), (pair_hbm, pair_ref), (comps_hbm, comps_ref),
            (gates_hbm, gates_ref), (x_hbm, x_ref), (w_hbm, w_ref), (table_hbm, table_ref)))
    ]
    for load in loads:
        load.start()
    barrier = pltpu.get_barrier_semaphore()
    loop(1, shards, lambda k: pl.semaphore_signal(
        barrier, inc=1, device_id=(g, lax.rem(s + k, shards)), device_id_type=MESH))
    loop(1, groups, lambda k: pl.semaphore_signal(
        barrier, inc=1, device_id=(lax.rem(g + k, groups), s), device_id_type=MESH))

    for load in loads[:5]:
        load.wait()

    target = owner_ref[...]
    slot = slot_ref[...]
    to_owner = jnp.where(iota((shards, n), 0) == target, 1.0, 0.0)
    earlier = ones_where(iota((n, n), 0) < iota((n, n), 1))
    before = nn(to_owner.astype(BF16), earlier)
    within = jnp.sum(before * to_owner, axis=0, keepdims=True).astype(jnp.int32)
    place_row = (target * CAP + within) * QUARTERS
    eye = iota((n, n), 0) == iota((n, n), 1)

    def as_column(row):
        wide = jnp.where(eye, row.astype(F32), 0.0)
        return jnp.sum(wide, axis=1, keepdims=True).astype(jnp.int32)

    place_col = as_column(place_row)
    wanted = (to_owner * (slot + 1).astype(F32)).astype(BF16)
    turn = ones_where(iota((LANES, n), 0) == within)
    head_send[...] = nt(wanted, turn).reshape(shards, 1, LANES)

    own_comps, gate_values = comps_ref[...].astype(F32), gates_ref[...].astype(F32)
    for u in range(CAP):
        for q in range(QUARTERS):
            row = u * QUARTERS + q
            own_rows[row:row + 1, :width] = own_comps[u:u + 1, q * width:(q + 1) * width]
    own_users[...] = own_rows[:, :width].astype(BF16)
    for pair in range(CAP // 2):
        own_gates[pair] = jnp.concatenate([gate_values[2 * pair:2 * pair + 1], gate_values[2 * pair + 1:2 * pair + 2]], axis=1)
    own = core * chips + x * nz + z
    users_all[block(own, BLOCK), :] = own_users[...]
    gate_rows = CAP // 2
    gates_all[pl.ds(own * gate_rows, gate_rows)] = own_gates[...]

    pl.semaphore_wait(barrier, shards - 1 + groups - 1)

    column = nx * CORES

    def head(away, p):
        return pltpu.make_async_remote_copy(
            src_ref=head_send.at[p], dst_ref=head_recv.at[s],
            send_sem=send_sems.at[0], recv_sem=head_sems.at[away],
            device_id=(g, p), device_id_type=MESH,
        )

    def send_head(k):
        p = lax.rem(s + k, shards)
        head(lax.rem(z - lax.div(p, column) + nz, nz), p).start()
    loop(1, shards, send_head)
    head_recv[s] = head_send[s]

    def send_users(k):
        p = lax.rem(chip + k, chips)
        copy(1, own_users, users_all.at[block(own, BLOCK)], (g, p * CORES + core)).start()
        copy(17, own_gates, gates_all.at[pl.ds(own * gate_rows, gate_rows)], (g, p * CORES + core)).start()
    loop(1, chips, send_users)
    loads[5].wait()

    for tile in range(d // LANES):
        turned = x_ref[:, tile * LANES:(tile + 1) * LANES].astype(F32).T.astype(BF16)
        for piece in range(max(1, LANES // depth)):
            size = min(depth, LANES)
            first = tile * LANES + piece * size
            holder, rest = divmod(first, depth)
            c_h, chip_h = holder % CORES, holder // CORES
            row = ((chip_h % nx) * nz + chip_h // nx) * depth + rest
            xt[c_h, row:row + size, :] = turned[piece * size:(piece + 1) * size]

    copy(2, xt.at[1 - core], xt_recv, partner).start()

    loads[6].wait()

    def tower(q):
        columns = block(q, width)
        pre = nn(x_ref[...], w_ref[:, columns])
        share = 0.5 + 0.5 * lax.erf(pre * (0.5 ** 0.5))
        embedded[block(q, n), :] = (pre * share).astype(BF16)
        slope[:, columns] = share + pre * (0.3989422804014327 * jnp.exp(-0.5 * pre * pre))
    loop(0, QUARTERS, tower)

    tile_rows = min(256, rows)
    span = column * BLOCK

    def answer(step):
        away = (step + 1) >> 1
        off = jnp.where((step & 1) == 1, away, nz - away)
        z_from = lax.rem(z + off, nz)
        first = z_from * column

        @pl.when(step == 0)
        def _():
            pltpu.make_async_copy(
                head_recv.at[pl.ds(0, column - 1)], head_recv.at[pl.ds(0, column - 1)], head_sems.at[0]).wait()

        @pl.when(step > 0)
        def _():
            whole = head_recv.at[pl.ds(0, column)]
            pltpu.make_async_copy(whole, whole, head_sems.at[lax.rem(off, nz)]).wait()

        heads = head_recv[pl.ds(first, column)].reshape(column, LANES).astype(BF16)
        spread = nn(ones_where((iota((span, column), 0) >> 4) == iota((span, column), 1)), heads)
        index = iota((span, LANES), 0)
        mine = jnp.where(((index >> 2) & 3) == iota((span, LANES), 1), spread, 0.0)
        asked = jnp.sum(mine, axis=1, keepdims=True).astype(jnp.int32) - 1
        quarter = index[:, 0:1] & 3
        out = jnp.zeros((span, width), F32)
        for q in range(QUARTERS):
            key = jnp.where(quarter == q, asked, -1)
            pick = ones_where(key == iota((span, slots), 1))
            out = out + nn(pick, table_ref[:, q * width:(q + 1) * width])
        rows_send[block(z_from, span), :] = out.astype(BF16)

        def send_rows(k):
            p = first + k

            @pl.when(p != s)
            def _():
                copy(3, rows_send.at[block(p, BLOCK)], rows_recv.at[block(s, BLOCK)], (g, p)).start()
        loop(0, column, send_rows)
    loads[7].wait()
    loop(0, nz, answer)
    rows_recv[block(s, BLOCK), :] = rows_send[block(s, BLOCK), :]

    others = pl.ds(0, half - BLOCK)
    wait_recv(1, users_all.at[others])
    mine = pl.ds(pl.multiple_of(core * half, half), half)
    copy(4, users_all.at[mine], users_all.at[mine], partner).start()
    other_gates = pl.ds(0, (chips - 1) * gate_rows)
    wait_recv(17, gates_all.at[other_gates])
    my_gates = pl.ds(core * chips * gate_rows, chips * gate_rows)
    copy(18, gates_all.at[my_gates], gates_all.at[my_gates], partner).start()

    heads = head_recv[...].reshape(shards, LANES).astype(BF16)
    held = tn(heads, ones_where((iota((shards, rows), 1) >> 4) == iota((shards, rows), 0)))
    lane = iota((LANES, rows), 1)
    held = jnp.where(((lane >> 2) & 3) == iota((LANES, rows), 0), held, 0.0)
    asked_row = jnp.sum(held, axis=0, keepdims=True).astype(jnp.int32) - 1

    def user_key(row):
        user, holder = row & 3, row >> 2
        c_u, chip_u = holder & 1, holder >> 1
        where = c_u * chips + (chip_u & (nx - 1)) * nz + (chip_u >> (nx.bit_length() - 1))
        return (where * CAP + user) * QUARTERS

    key_rows = [user_key(pair_ref[side:side + 1, :]) for side in range(2)]
    key_cols = [as_column(row) for row in key_rows]
    gate = iota((LANES, width), 0)
    expand = ones_where((gate < COMPS * COMPS) & ((gate & 15) == (iota((LANES, width), 1) >> 4)))
    wait_recv(4, users_all.at[mine])
    wait_recv(18, gates_all.at[my_gates])
    gate_table = gates_all[...].reshape(shards * gate_rows, LANES).astype(BF16)
    gate_lane = iota((LANES, width), 0)
    gate_of = (gate_lane & 15) == (iota((LANES, width), 1) >> 4)
    for side in range(2):
        user = key_cols[side] >> 2
        taken = nn(ones_where((user >> 1) == iota((n, shards * gate_rows), 1)), gate_table)
        taken = jnp.where((iota((n, LANES), 1) >> 6) == (user & 1), taken, 0.0).astype(BF16)

        def pick_users(q):
            pick = ones_where(key_cols[side] + q == iota((n, rows), 1))
            here = block(side * QUARTERS + q, n)
            picked[here, :] = nn(pick, users_all[...]).astype(BF16)
            part = ones_where(gate_of & (((gate_lane & 63) >> 4) == q))
            gates_wide[here, :] = nn(taken, part).astype(BF16)
        loop(0, QUARTERS, pick_users)

    wait_recv(3, rows_recv.at[pl.ds(0, rows - BLOCK)])

    def combine(q):
        pick = ones_where(place_col + q == iota((n, rows), 1))
        here = block(q, n)
        combined[here, :] = embedded[here, :].astype(F32) + nn(pick, rows_recv[...])
    loop(0, QUARTERS, combine)

    def spot(index, b):
        return pl.ds(pl.multiple_of(index * n + b * GROUP, GROUP), GROUP)

    def lanes_of(p):
        return slice((p & 1) * LANES, (p & 1) * LANES + LANES)

    def stack(ref, b, sides):
        return jnp.concatenate(
            [ref[spot(side * QUARTERS + (p >> 1), b), lanes_of(p)] for side in range(sides) for p in range(COMPS)],
            axis=0)

    pairs = COMPS * GROUP

    def pair_loss(b):
        stores = []

        def store(ref, where, lanes, values):
            stores.append((ref, where, lanes, values))

        comb = stack(combined, b, 1)
        scale = lax.rsqrt(jnp.mean(comb * comb, axis=1, keepdims=True) + 1e-06)
        normed = comb * scale
        n_high, n_low = halves(normed)
        users = stack(picked, b, 2)
        gates = stack(gates_wide, b, 2).astype(F32)
        logits = nt(users, n_high) + nt(users, n_low)
        same = (iota((2 * pairs, pairs), 0) & (GROUP - 1)) == (iota((2 * pairs, pairs), 1) & (GROUP - 1))
        weights = sigmoid(gates + logits)
        terms = jnp.where(same, weights * logits, 0.0)
        factors = []
        for side in range(2):
            total = terms[side * pairs:side * pairs + GROUP]
            for p in range(1, COMPS):
                total = total + terms[side * pairs + p * GROUP:side * pairs + (p + 1) * GROUP]
            score = 0.125 * jnp.sum(total, axis=1, keepdims=True)
            factor = sigmoid(score) if side else -sigmoid(-score)
            factors += [0.125 * factor] * COMPS
        factor = jnp.where(same, jnp.concatenate(factors, axis=0), 0.0)
        bend = logits * (weights * (1.0 - weights))
        dg_high, dg_low = halves(factor * bend)
        dl = factor * (weights + bend)
        dl_high, dl_low = halves(dl)
        d_normed = tn(dl_high, users) + tn(dl_low, users)
        du_high, du_low = halves(nn(dl_high, n_high) + nn(dl_low, n_high) + nn(dl_high, n_low))
        d_row = scale * (d_normed - normed * jnp.mean(d_normed * normed, axis=1, keepdims=True))
        d_row = d_row.astype(BF16)
        for p in range(COMPS):
            part = d_row[p * GROUP:(p + 1) * GROUP]
            store(d_comb, spot(p >> 1, b), lanes_of(p), part)
            item, column = block(b, GROUP), slice(p * LANES, (p + 1) * LANES)
            store(d_pre, item, column, (part.astype(F32) * slope[item, column]).astype(BF16))
        for side in range(2):
            for p in range(COMPS):
                here = spot(side * QUARTERS + (p >> 1), b)
                part = slice(side * pairs + p * GROUP, side * pairs + (p + 1) * GROUP)
                lane0 = (p & 1) * LANES
                store(d_users, here, slice(lane0, lane0 + LANES), du_high[part])
                store(d_users, here, slice(width + lane0, width + lane0 + LANES), du_low[part])
                store(d_gates, here, slice(lane0, lane0 + LANES), dg_high[part])
                store(d_gates, here, slice(width + lane0, width + lane0 + LANES), dg_low[part])
        return stores

    together = 2 - (n // GROUP) % 2

    def pair_losses(t):
        for stores in [pair_loss(t * together + i) for i in range(together)]:
            for ref, where, lanes, values in stores:
                ref[where, lanes] = values
    loop(0, n // (GROUP * together), pair_losses)

    copy(5, d_pre, d_pre_recv, partner).start()

    def give_back(t):
        index = iota((tile_rows, n), 0) + t * tile_rows
        put = jnp.concatenate([ones_where(index == place_row + q) for q in range(QUARTERS)], axis=1)
        back_send[block(t, tile_rows), :] = nn(put, d_comb[...]).astype(BF16)
    loop(0, rows // tile_rows, give_back)

    first = tower_part.shape[1]
    deep = nx * depth
    wait_recv(2, xt_recv)
    wait_recv(5, d_pre_recv)
    wide = nz * depth

    def tower_rows(i):
        here = block(i, wide)
        total = nn(xt[core, here, :], d_pre[...]) + nn(xt_recv[here, :], d_pre_recv[...])
        tower_part[here, :] = total[:, :first].astype(BF16)
        for j in range(nz):
            there = pl.ds(pl.multiple_of((j * nx + i) * depth, depth), depth)
            other_part[there, :] = total[j * depth:(j + 1) * depth, first:].astype(BF16)
    loop(0, nx, tower_rows)

    def send_x(k):
        to = lax.rem(x + k, nx)
        copy(8, tower_part.at[block(to, wide)], tower_x.at[x], at(z, to, core)).start()
    loop(1, nx, send_x)

    def send_other_y(k):
        to = lax.rem(g + k, groups)
        copy(13, other_part.at[block(to, deep)], other_y.at[g], (to, s)).start()
    loop(1, groups, send_other_y)

    far = max(1, 3 * nz // 8)

    def send_back(step):
        away = (step + 1) >> 1
        z_to = lax.rem(z + nz // 2 + jnp.where((step & 1) == 1, nz - away, away), nz)

        def send_one(k):
            p = z_to * column + k

            @pl.when(p != s)
            def _():
                copy(6, back_send.at[block(p, BLOCK)], back_recv.at[block(s, BLOCK)], (g, p)).start()
        loop(0, column, send_one)
    loop(0, far, send_back)
    back_recv[block(s, BLOCK), :] = back_send[block(s, BLOCK), :]

    def squeeze(i):
        here = block(i, n)
        high, low = halves(nt(d_gates[here, :width], expand) + nt(d_gates[here, width:], expand))
        ours = (iota((n, LANES), 1) >> 4) == (i & 3)
        zero = jnp.zeros((n, LANES), BF16)
        d_users[here, 2 * width:2 * width + LANES] = jnp.where(ours, high, zero)
        d_users[here, 2 * width + LANES:] = jnp.where(ours, low, zero)
    loop(0, 2 * QUARTERS, squeeze)

    tile_users = min(128, rows)

    def sum_users(t):
        index = iota((tile_users, n), 0) + t * tile_users
        put = jnp.concatenate(
            [ones_where(index == key_rows[side] + q) for side in range(2) for q in range(QUARTERS)], axis=1)
        total = nn(put, d_users[...])
        here = block(t, tile_users)
        users_part[here, :width] = total[:, :width] + total[:, width:2 * width]
        users_part[here, width:] = total[:, 2 * width:2 * width + LANES] + total[:, 2 * width + LANES:]
    loop(0, rows // tile_users, sum_users)
    theirs = pl.ds(pl.multiple_of((1 - core) * half, half), half)
    copy(7, users_part.at[theirs], users_part_recv, partner).start()
    wait_recv(7, users_part_recv)
    users_half[...] = (users_part[mine, :] + users_part_recv[...]).astype(BF16)
    tall = nz * BLOCK

    def send_ux(k):
        to = lax.rem(x + k, nx)
        copy(9, users_half.at[block(to, tall)], users_x.at[x], at(z, to, core)).start()
    loop(1, nx, send_ux)

    wait_recv(8, tower_x.at[pl.ds(0, nx - 1)])
    total = tower_part[block(x, wide), :].astype(F32)
    for k in range(1, nx):
        total = total + tower_x[lax.rem(x + k, nx)].astype(F32)
    tower_mid[...] = total.astype(BF16)

    def send_z(k):
        to = lax.rem(z + k, nz)
        copy(10, tower_mid.at[block(to, depth)], tower_z.at[z], at(to, x, core)).start()
    loop(1, nz, send_z)
    loop(far, nz, send_back)

    wait_recv(13, other_y.at[pl.ds(0, groups - 1)])
    total = other_part[block(g, deep), :].astype(F32)
    for k in range(1, groups):
        total = total + other_y[lax.rem(g + k, groups)].astype(F32)
    other_mid[...] = total.astype(BF16)

    def send_other_x(k):
        to = lax.rem(x + k, nx)
        copy(14, other_mid.at[block(to, depth)], other_x.at[x], at(z, to, core)).start()
    loop(1, nx, send_other_x)

    wait_recv(9, users_x.at[pl.ds(0, nx - 1)])
    total = users_half[block(x, tall), :].astype(F32)
    for k in range(1, nx):
        total = total + users_x[lax.rem(x + k, nx)].astype(F32)
    users_mid[...] = total.astype(BF16)

    def send_uz(k):
        to = lax.rem(z + k, nz)
        copy(11, users_mid.at[block(to, BLOCK)], users_z.at[z], at(to, x, core)).start()
    loop(1, nz, send_uz)

    wait_recv(14, other_x.at[pl.ds(0, nx - 1)])
    total = other_mid[block(x, depth), :].astype(F32)
    for k in range(1, nx):
        total = total + other_x[lax.rem(x + k, nx)].astype(F32)
    other_low[...] = total

    @pl.when(z != g)
    def _():
        copy(15, other_low, other_z.at[z], at(g, x, core)).start()

    wait_recv(10, tower_z.at[pl.ds(0, nz - 1)])
    total = tower_mid[block(z, depth), :].astype(F32)
    for k in range(1, nz):
        total = total + tower_z[lax.rem(z + k, nz)].astype(F32)
    tower_low[...] = total.astype(BF16)

    def send_y(k):
        copy(12, tower_low, tower_y.at[g], (lax.rem(g + k, groups), s)).start()
    loop(1, groups, send_y)

    @pl.when(z == g)
    def _():
        wait_recv(15, other_z.at[pl.ds(0, nz - 1)])
        total = other_low[...]
        for k in range(1, nz):
            total = total + other_z[lax.rem(z + k, nz)]
        other_got[...] = total.astype(BF16)

        def send_other(k):
            copy(16, other_got, other_got, (lax.rem(g + k, groups), s)).start()
        loop(1, groups, send_other)

    wait_recv(6, back_recv.at[pl.ds(0, rows - BLOCK)])
    quarter_row = iota((1, rows), 1) & 3
    for q in range(QUARTERS):
        key = jnp.where(quarter_row == q, asked_row, -1)
        pick = ones_where(key == iota((slots, rows), 0))
        table_out[:, q * width:(q + 1) * width] = nn(pick, back_recv[...])

    wait_recv(11, users_z.at[pl.ds(0, nz - 1)])
    total = users_mid[block(z, BLOCK), :].astype(F32)
    for k in range(1, nz):
        total = total + users_z[lax.rem(z + k, nz)].astype(F32)
    own_rows[...] = total
    for u in range(CAP):
        gate_row = jnp.zeros((1, COMPS * COMPS), F32)
        for q in range(QUARTERS):
            row = u * QUARTERS + q
            users_out[u:u + 1, q * width:(q + 1) * width] = own_rows[row:row + 1, :width]
            gate_row = gate_row + own_rows[row:row + 1, width:width + COMPS * COMPS]
        gates_out[u:u + 1, :] = gate_row

    tower_y[g] = tower_low[...]
    wait_recv(12, tower_y.at[pl.ds(0, groups - 1)])
    total = tower_y[0].astype(F32)
    for k in range(1, groups):
        total = total + tower_y[k].astype(F32)
    tower_out[:, :first] = total

    @pl.when(z != g)
    def _():
        wait_recv(16, other_got)
        wait_send(15, other_low)

    @pl.when(z == g)
    def _():
        wait_send(16, other_part.at[pl.ds(0, (groups - 1) * depth)])

    tower_out[:, first:] = other_got[...].astype(F32)
    wait_send(13, other_y.at[pl.ds(0, groups - 1)])
    wait_send(14, other_x.at[pl.ds(0, nx - 1)])

    wait_send(0, head_send.at[pl.ds(0, shards - 1)])
    wait_send(1, users_all.at[others])
    wait_send(17, gates_all.at[other_gates])
    wait_send(18, gates_all.at[my_gates])
    wait_send(2, xt_recv)
    wait_send(3, rows_send.at[pl.ds(0, rows - BLOCK)])
    wait_send(4, users_all.at[mine])
    wait_send(5, d_pre)
    wait_send(6, back_send.at[pl.ds(0, rows - BLOCK)])
    wait_send(7, users_part_recv)
    wait_send(8, tower_x.at[pl.ds(0, nx - 1)])
    wait_send(9, users_x.at[pl.ds(0, nx - 1)])
    wait_send(10, tower_z.at[pl.ds(0, nz - 1)])
    wait_send(11, users_z.at[pl.ds(0, nz - 1)])
    wait_send(12, tower_y.at[pl.ds(0, groups - 1)])


def local(item_features, tower_weight, item_table, owner, table_slot, pair_users, user_comps, user_gates):
    groups, shards = lax.axis_size("group"), lax.axis_size("shard")
    nx = 4 if shards >= 64 else 2
    nz = shards // (nx * CORES)
    n, d = item_features.shape
    slots = item_table.shape[0]
    held = user_comps.shape[0]
    width = d // QUARTERS
    rows = shards * BLOCK
    half = rows // CORES
    depth = d // shards
    across = width + LANES
    first = d * 5 // 8
    other = d - first
    assert groups == nz
    scratch = [
        ((1, n), jnp.int32), ((1, n), jnp.int32), ((2, n), jnp.int32), ((held, d), BF16), ((held, COMPS * COMPS), BF16),
        ((n, d), BF16), ((d, d), BF16), ((slots, d), BF16),
        ((BLOCK, across), F32), ((BLOCK, width), BF16), ((CAP // 2, 1, LANES), F32), ((shards * CAP // 2, 1, LANES), F32),
        ((shards, 1, LANES), F32), ((shards, 1, LANES), F32),
        ((rows, width), BF16),
        ((CORES, d // 2, n), BF16), ((d // 2, n), BF16),
        ((QUARTERS * n, width), BF16), ((n, d), F32),
        ((rows, width), BF16), ((rows, width), BF16),
        ((2 * QUARTERS * n, width), BF16), ((2 * QUARTERS * n, width), BF16),
        ((QUARTERS * n, width), F32), ((QUARTERS * n, width), BF16),
        ((n, d), BF16), ((n, d), BF16),
        ((2 * QUARTERS * n, 2 * across), BF16), ((2 * QUARTERS * n, 2 * width), BF16),
        ((rows, across), F32), ((half, across), F32),
        ((d // 2, first), BF16), ((nx, nz * depth, first), BF16), ((nz * depth, first), BF16),
        ((nz, depth, first), BF16), ((depth, first), BF16), ((groups, depth, first), BF16),
        ((d // 2, other), BF16), ((groups, nx * depth, other), BF16), ((nx * depth, other), BF16),
        ((nx, depth, other), BF16), ((depth, other), F32), ((nz, depth, other), F32), ((depth, other), BF16),
        ((half, across), BF16), ((nx, nz * BLOCK, across), BF16), ((nz * BLOCK, across), BF16),
        ((nz, BLOCK, across), BF16),
        ((rows, width), BF16), ((rows, width), BF16),
    ]
    whole = pl.BlockSpec(memory_space=pltpu.VMEM)
    return pl.pallas_call(
        functools.partial(kernel, groups, shards, nx),
        out_shape=(
            jax.ShapeDtypeStruct((depth, d), F32),
            jax.ShapeDtypeStruct((slots, d), F32),
            jax.ShapeDtypeStruct((held, d), F32),
            jax.ShapeDtypeStruct((held, COMPS * COMPS), F32),
        ),
        in_specs=[pl.BlockSpec(memory_space=pltpu.HBM)] * 8,
        out_specs=(whole,) * 4,
        scratch_shapes=[pltpu.VMEM(shape, kind) for shape, kind in scratch]
        + [pltpu.SemaphoreType.DMA((19,)), pltpu.SemaphoreType.DMA((19,)), pltpu.SemaphoreType.DMA((nz,)),
           pltpu.SemaphoreType.DMA((8,))],
        compiler_params=pltpu.CompilerParams(
            collective_id=0, has_side_effects=True, vmem_limit_bytes=32 * 1024 * 1024),
    )(*(pltpu.with_memory_space_constraint(a, pltpu.HBM) for a in (
        owner.reshape(1, n), table_slot.reshape(1, n), pair_users.T, user_comps, user_gates,
        item_features, tower_weight, item_table)))


def solution(mesh):
    spread = P(("group", "shard"), None)
    return jax.shard_map(
        local,
        mesh=mesh,
        in_specs=(spread, P(), spread, spread, P(("group", "shard")), spread, spread, spread),
        out_specs=(P("shard", None), spread, spread, spread),
        check_vma=False,
    )
```

```python
import functools

import jax
import jax.numpy as jnp
from jax import lax
from jax.experimental import pallas as pl
from jax.experimental.pallas import tpu as pltpu
from jax.sharding import PartitionSpec as P

MESH = pl.DeviceIdType.MESH
COMPS = 8
CAP = 4
CORES = 2
QUARTERS = 4
BLOCK = CAP * QUARTERS
GROUP = 16
LANES = 128
F32, BF16 = jnp.float32, jnp.bfloat16


def nn(a, b):
    return lax.dot_general(a, b, (((1,), (0,)), ((), ())), preferred_element_type=F32)


def nt(a, b):
    return lax.dot_general(a, b, (((1,), (1,)), ((), ())), preferred_element_type=F32)


def tn(a, b):
    return lax.dot_general(a, b, (((0,), (0,)), ((), ())), preferred_element_type=F32)


def ones_where(condition):
    return jnp.where(condition, 1.0, 0.0).astype(BF16)


def iota(shape, dim):
    return lax.broadcasted_iota(jnp.int32, shape, dim)


def halves(values):
    high = values.astype(BF16)
    return high, (values - high.astype(F32)).astype(BF16)


def sigmoid(values):
    return 1.0 / (1.0 + jnp.exp(-values))


def kernel(
    groups, shards, nx,
    owner_hbm, slot_hbm, pair_hbm, comps_hbm, gates_hbm, x_hbm, w_hbm, table_hbm,
    tower_out, table_out, users_out, gates_out,
    owner_ref, slot_ref, pair_ref, comps_ref, gates_ref, x_ref, w_ref, table_ref,
    own_rows, own_users, own_gates, gates_all, head_send, head_recv, users_all, xt, xt_recv, embedded, slope, rows_send, rows_recv,
    picked, gates_wide, combined, d_comb, d_pre, d_pre_recv, d_users, d_gates,
    users_part, users_part_recv, tower_part, tower_x, tower_mid, tower_z, tower_low, tower_y,
    other_part, other_y, other_mid, other_x, other_low, other_z, other_got,
    users_half, users_x, users_mid, users_z, back_send, back_recv,
    send_sems, recv_sems, head_sems, load_sems,
):
    n, d = x_ref.shape
    slots = table_ref.shape[0]
    width = d // QUARTERS
    rows = shards * BLOCK
    half = rows // CORES
    nz = shards // (nx * CORES)
    depth = d // shards
    chips = shards // CORES
    g, s = lax.axis_index("group"), lax.axis_index("shard")
    core = lax.rem(s, CORES)
    chip = lax.div(s, CORES)
    x, z = lax.rem(chip, nx), lax.div(chip, nx)

    def at(z_to, x_to, core_to):
        return (g, (z_to * nx + x_to) * CORES + core_to)

    partner = at(z, x, 1 - core)

    def copy(number, source, target, device):
        return pltpu.make_async_remote_copy(
            src_ref=source, dst_ref=target,
            send_sem=send_sems.at[number], recv_sem=recv_sems.at[number],
            device_id=device, device_id_type=MESH,
        )

    def wait_recv(number, whole):
        copy(number, whole, whole, partner).wait_recv()

    def wait_send(number, whole):
        copy(number, whole, whole, partner).wait_send()

    def loop(low, high, step):
        def run(i, carry):
            step(i)
            return carry
        lax.fori_loop(low, high, run, 0)

    def block(i, size):
        return pl.ds(pl.multiple_of(i * size, size), size)

    loads = [
        pltpu.make_async_copy(source, target, load_sems.at[i])
        for i, (source, target) in enumerate((
            (owner_hbm, owner_ref), (slot_hbm, slot_ref), (pair_hbm, pair_ref), (comps_hbm, comps_ref),
            (gates_hbm, gates_ref), (x_hbm, x_ref), (w_hbm, w_ref), (table_hbm, table_ref)))
    ]
    for load in loads:
        load.start()
    barrier = pltpu.get_barrier_semaphore()
    column = nx * CORES

    def far_first(low, high, step):
        def at_distance(turn):
            away = (turn + 1) >> 1
            z_to = lax.rem(z + nz // 2 + jnp.where((turn & 1) == 1, nz - away, away), nz)

            def one(k):
                p = z_to * column + k

                @pl.when(p != s)
                def _():
                    step(p, z_to)
            loop(0, column, one)
        loop(low, high, at_distance)

    far_first(0, nz, lambda p, z_to: pl.semaphore_signal(
        barrier, inc=1, device_id=(g, p), device_id_type=MESH))
    loop(1, groups, lambda k: pl.semaphore_signal(
        barrier, inc=1, device_id=(lax.rem(g + k, groups), s), device_id_type=MESH))

    for load in loads[:5]:
        load.wait()

    target = owner_ref[...]
    slot = slot_ref[...]
    to_owner = jnp.where(iota((shards, n), 0) == target, 1.0, 0.0)
    earlier = ones_where(iota((n, n), 0) < iota((n, n), 1))
    before = nn(to_owner.astype(BF16), earlier)
    within = jnp.sum(before * to_owner, axis=0, keepdims=True).astype(jnp.int32)
    place_row = (target * CAP + within) * QUARTERS
    eye = iota((n, n), 0) == iota((n, n), 1)

    def as_column(row):
        wide = jnp.where(eye, row.astype(F32), 0.0)
        return jnp.sum(wide, axis=1, keepdims=True).astype(jnp.int32)

    place_col = as_column(place_row)
    wanted = (to_owner * (slot + 1).astype(F32)).astype(BF16)
    turn = ones_where(iota((LANES, n), 0) == within)
    head_send[...] = nt(wanted, turn).reshape(shards, 1, LANES)

    own_comps, gate_values = comps_ref[...].astype(F32), gates_ref[...].astype(F32)
    for u in range(CAP):
        for q in range(QUARTERS):
            row = u * QUARTERS + q
            own_rows[row:row + 1, :width] = own_comps[u:u + 1, q * width:(q + 1) * width]
    own_users[...] = own_rows[:, :width].astype(BF16)
    for pair in range(CAP // 2):
        own_gates[pair] = jnp.concatenate([gate_values[2 * pair:2 * pair + 1], gate_values[2 * pair + 1:2 * pair + 2]], axis=1)
    own = core * chips + x * nz + z
    users_all[block(own, BLOCK), :] = own_users[...]
    gate_rows = CAP // 2
    gates_all[pl.ds(own * gate_rows, gate_rows)] = own_gates[...]

    pl.semaphore_wait(barrier, shards - 1 + groups - 1)

    def head(away, p):
        return pltpu.make_async_remote_copy(
            src_ref=head_send.at[p], dst_ref=head_recv.at[s],
            send_sem=send_sems.at[0], recv_sem=head_sems.at[away],
            device_id=(g, p), device_id_type=MESH,
        )

    far_first(0, nz, lambda p, z_to: head(lax.rem(z - z_to + nz, nz), p).start())
    head_recv[s] = head_send[s]

    def send_users(k):
        p = lax.rem(chip + k, chips)
        ahead = lax.rem(lax.div(p, nx) - z + nz, nz)

        @pl.when((ahead <= 2) | (ahead >= nz - 2))
        def _():
            copy(1, own_users, users_all.at[block(own, BLOCK)], (g, p * CORES + core)).start()
        copy(17, own_gates, gates_all.at[pl.ds(own * gate_rows, gate_rows)], (g, p * CORES + core)).start()
    loop(1, chips, send_users)
    loads[5].wait()

    for tile in range(d // LANES):
        turned = x_ref[:, tile * LANES:(tile + 1) * LANES].astype(F32).T.astype(BF16)
        for piece in range(max(1, LANES // depth)):
            size = min(depth, LANES)
            first = tile * LANES + piece * size
            holder, rest = divmod(first, depth)
            c_h, chip_h = holder % CORES, holder // CORES
            row = ((chip_h % nx) * nz + chip_h // nx) * depth + rest
            xt[c_h, row:row + size, :] = turned[piece * size:(piece + 1) * size]

    copy(2, xt.at[1 - core], xt_recv, partner).start()

    loads[6].wait()

    def tower(q):
        columns = block(q, width)
        pre = nn(x_ref[...], w_ref[:, columns])
        share = 0.5 + 0.5 * lax.erf(pre * (0.5 ** 0.5))
        embedded[block(q, n), :] = (pre * share).astype(BF16)
        slope[:, columns] = share + pre * (0.3989422804014327 * jnp.exp(-0.5 * pre * pre))
    loop(0, QUARTERS, tower)

    direct = min(5, nz) * nx - 1
    wait_recv(1, users_all.at[pl.ds(0, direct * BLOCK)])

    def relay(z_from, z_to, x_low, x_high):
        def one(k):
            here = block(core * chips + k * nz + z_from, BLOCK)
            copy(19, users_all.at[here], users_all.at[here], at(z_to, x, core)).start()
        loop(x_low, x_high, one)

    relayed = (nz - min(5, nz)) * nx
    if relayed:
        up, down = lax.rem(z + 2, nz), lax.rem(z + nz - 2, nz)
        relay(down, lax.rem(z + 1, nz), 0, nx)
        relay(up, lax.rem(z + nz - 1, nz), 0, nx)
        relay(down, up, 0, nx // 2)
        relay(up, down, nx // 2, nx)

    tile_rows = min(256, rows)
    span = column * BLOCK

    def answer(step):
        away = (step + 1) >> 1
        off = jnp.where((step & 1) == 1, away, nz - away)
        z_from = lax.rem(z + off, nz)
        first = z_from * column

        @pl.when(step == 0)
        def _():
            pltpu.make_async_copy(
                head_recv.at[pl.ds(0, column - 1)], head_recv.at[pl.ds(0, column - 1)], head_sems.at[0]).wait()

        @pl.when(step > 0)
        def _():
            whole = head_recv.at[pl.ds(0, column)]
            pltpu.make_async_copy(whole, whole, head_sems.at[lax.rem(off, nz)]).wait()

        heads = head_recv[pl.ds(first, column)].reshape(column, LANES).astype(BF16)
        spread = nn(ones_where((iota((span, column), 0) >> 4) == iota((span, column), 1)), heads)
        index = iota((span, LANES), 0)
        mine = jnp.where(((index >> 2) & 3) == iota((span, LANES), 1), spread, 0.0)
        asked = jnp.sum(mine, axis=1, keepdims=True).astype(jnp.int32) - 1
        quarter = index[:, 0:1] & 3
        out = jnp.zeros((span, width), F32)
        for q in range(QUARTERS):
            key = jnp.where(quarter == q, asked, -1)
            pick = ones_where(key == iota((span, slots), 1))
            out = out + nn(pick, table_ref[:, q * width:(q + 1) * width])
        rows_send[block(z_from, span), :] = out.astype(BF16)

        def send_rows(k):
            p = first + k

            @pl.when(p != s)
            def _():
                copy(3, rows_send.at[block(p, BLOCK)], rows_recv.at[block(s, BLOCK)], (g, p)).start()
        loop(0, column, send_rows)
    loads[7].wait()
    loop(0, nz, answer)
    rows_recv[block(s, BLOCK), :] = rows_send[block(s, BLOCK), :]

    if relayed:
        wait_recv(19, users_all.at[pl.ds(0, relayed * BLOCK)])
    mine = pl.ds(pl.multiple_of(core * half, half), half)
    copy(4, users_all.at[mine], users_all.at[mine], partner).start()
    other_gates = pl.ds(0, (chips - 1) * gate_rows)
    wait_recv(17, gates_all.at[other_gates])
    my_gates = pl.ds(core * chips * gate_rows, chips * gate_rows)
    copy(18, gates_all.at[my_gates], gates_all.at[my_gates], partner).start()

    heads = head_recv[...].reshape(shards, LANES).astype(BF16)
    held = tn(heads, ones_where((iota((shards, rows), 1) >> 4) == iota((shards, rows), 0)))
    lane = iota((LANES, rows), 1)
    held = jnp.where(((lane >> 2) & 3) == iota((LANES, rows), 0), held, 0.0)
    asked_row = jnp.sum(held, axis=0, keepdims=True).astype(jnp.int32) - 1

    def user_key(row):
        user, holder = row & 3, row >> 2
        c_u, chip_u = holder & 1, holder >> 1
        where = c_u * chips + (chip_u & (nx - 1)) * nz + (chip_u >> (nx.bit_length() - 1))
        return (where * CAP + user) * QUARTERS

    key_rows = [user_key(pair_ref[side:side + 1, :]) for side in range(2)]
    key_cols = [as_column(row) for row in key_rows]
    gate = iota((LANES, width), 0)
    expand = ones_where((gate < COMPS * COMPS) & ((gate & 15) == (iota((LANES, width), 1) >> 4)))
    wait_recv(4, users_all.at[mine])
    wait_recv(18, gates_all.at[my_gates])
    gate_table = gates_all[...].reshape(shards * gate_rows, LANES).astype(BF16)
    gate_lane = iota((LANES, width), 0)
    gate_of = (gate_lane & 15) == (iota((LANES, width), 1) >> 4)
    for side in range(2):
        user = key_cols[side] >> 2
        taken = nn(ones_where((user >> 1) == iota((n, shards * gate_rows), 1)), gate_table)
        taken = jnp.where((iota((n, LANES), 1) >> 6) == (user & 1), taken, 0.0).astype(BF16)

        def pick_users(q):
            pick = ones_where(key_cols[side] + q == iota((n, rows), 1))
            here = block(side * QUARTERS + q, n)
            picked[here, :] = nn(pick, users_all[...]).astype(BF16)
            part = ones_where(gate_of & (((gate_lane & 63) >> 4) == q))
            gates_wide[here, :] = nn(taken, part).astype(BF16)
        loop(0, QUARTERS, pick_users)

    wait_recv(3, rows_recv.at[pl.ds(0, rows - BLOCK)])

    def combine(q):
        pick = ones_where(place_col + q == iota((n, rows), 1))
        here = block(q, n)
        combined[here, :] = embedded[here, :].astype(F32) + nn(pick, rows_recv[...])
    loop(0, QUARTERS, combine)

    def spot(index, b):
        return pl.ds(pl.multiple_of(index * n + b * GROUP, GROUP), GROUP)

    def lanes_of(p):
        return slice((p & 1) * LANES, (p & 1) * LANES + LANES)

    def stack(ref, b, sides):
        return jnp.concatenate(
            [ref[spot(side * QUARTERS + (p >> 1), b), lanes_of(p)] for side in range(sides) for p in range(COMPS)],
            axis=0)

    pairs = COMPS * GROUP

    def pair_loss(b):
        stores = []

        def store(ref, where, lanes, values):
            stores.append((ref, where, lanes, values))

        comb = stack(combined, b, 1)
        scale = lax.rsqrt(jnp.mean(comb * comb, axis=1, keepdims=True) + 1e-06)
        normed = comb * scale
        n_high, n_low = halves(normed)
        users = stack(picked, b, 2)
        gates = stack(gates_wide, b, 2).astype(F32)
        logits = nt(users, n_high) + nt(users, n_low)
        same = (iota((2 * pairs, pairs), 0) & (GROUP - 1)) == (iota((2 * pairs, pairs), 1) & (GROUP - 1))
        weights = sigmoid(gates + logits)
        terms = jnp.where(same, weights * logits, 0.0)
        factors = []
        for side in range(2):
            total = terms[side * pairs:side * pairs + GROUP]
            for p in range(1, COMPS):
                total = total + terms[side * pairs + p * GROUP:side * pairs + (p + 1) * GROUP]
            score = 0.125 * jnp.sum(total, axis=1, keepdims=True)
            factor = sigmoid(score) if side else -sigmoid(-score)
            factors += [0.125 * factor] * COMPS
        factor = jnp.where(same, jnp.concatenate(factors, axis=0), 0.0)
        bend = logits * (weights * (1.0 - weights))
        dg_high, dg_low = halves(factor * bend)
        dl = factor * (weights + bend)
        dl_high, dl_low = halves(dl)
        d_normed = tn(dl_high, users) + tn(dl_low, users)
        du_high, du_low = halves(nn(dl_high, n_high) + nn(dl_low, n_high) + nn(dl_high, n_low))
        d_row = scale * (d_normed - normed * jnp.mean(d_normed * normed, axis=1, keepdims=True))
        d_row = d_row.astype(BF16)
        for p in range(COMPS):
            part = d_row[p * GROUP:(p + 1) * GROUP]
            store(d_comb, spot(p >> 1, b), lanes_of(p), part)
            item, column = block(b, GROUP), slice(p * LANES, (p + 1) * LANES)
            store(d_pre, item, column, (part.astype(F32) * slope[item, column]).astype(BF16))
        for side in range(2):
            for p in range(COMPS):
                here = spot(side * QUARTERS + (p >> 1), b)
                part = slice(side * pairs + p * GROUP, side * pairs + (p + 1) * GROUP)
                lane0 = (p & 1) * LANES
                store(d_users, here, slice(lane0, lane0 + LANES), du_high[part])
                store(d_users, here, slice(width + lane0, width + lane0 + LANES), du_low[part])
                store(d_gates, here, slice(lane0, lane0 + LANES), dg_high[part])
                store(d_gates, here, slice(width + lane0, width + lane0 + LANES), dg_low[part])
        return stores

    together = 2 - (n // GROUP) % 2

    def pair_losses(t):
        for stores in [pair_loss(t * together + i) for i in range(together)]:
            for ref, where, lanes, values in stores:
                ref[where, lanes] = values
    loop(0, n // (GROUP * together), pair_losses)

    copy(5, d_pre, d_pre_recv, partner).start()

    def give_back(t):
        index = iota((tile_rows, n), 0) + t * tile_rows
        put = jnp.concatenate([ones_where(index == place_row + q) for q in range(QUARTERS)], axis=1)
        back_send[block(t, tile_rows), :] = nn(put, d_comb[...]).astype(BF16)
    loop(0, rows // tile_rows, give_back)

    first = tower_part.shape[1]
    deep = nx * depth
    wait_recv(2, xt_recv)
    wait_recv(5, d_pre_recv)
    wide = nz * depth

    def tower_rows(i):
        here = block(i, wide)
        total = nn(xt[core, here, :], d_pre[...]) + nn(xt_recv[here, :], d_pre_recv[...])
        tower_part[here, :] = total[:, :first].astype(BF16)
        for j in range(nz):
            there = pl.ds(pl.multiple_of((j * nx + i) * depth, depth), depth)
            other_part[there, :] = total[j * depth:(j + 1) * depth, first:].astype(BF16)
    loop(0, nx, tower_rows)

    def send_x(k):
        to = lax.rem(x + k, nx)
        copy(8, tower_part.at[block(to, wide)], tower_x.at[x], at(z, to, core)).start()
    loop(1, nx, send_x)

    def send_other_y(k):
        to = lax.rem(g + k, groups)
        copy(13, other_part.at[block(to, deep)], other_y.at[g], (to, s)).start()
    loop(1, groups, send_other_y)

    far = max(1, 3 * nz // 8)

    def send_back(p, z_to):
        copy(6, back_send.at[block(p, BLOCK)], back_recv.at[block(s, BLOCK)], (g, p)).start()
    far_first(0, far, send_back)
    back_recv[block(s, BLOCK), :] = back_send[block(s, BLOCK), :]

    def squeeze(i):
        here = block(i, n)
        high, low = halves(nt(d_gates[here, :width], expand) + nt(d_gates[here, width:], expand))
        ours = (iota((n, LANES), 1) >> 4) == (i & 3)
        zero = jnp.zeros((n, LANES), BF16)
        d_users[here, 2 * width:2 * width + LANES] = jnp.where(ours, high, zero)
        d_users[here, 2 * width + LANES:] = jnp.where(ours, low, zero)
    loop(0, 2 * QUARTERS, squeeze)

    tile_users = min(128, rows)

    def sum_users(t):
        index = iota((tile_users, n), 0) + t * tile_users
        put = jnp.concatenate(
            [ones_where(index == key_rows[side] + q) for side in range(2) for q in range(QUARTERS)], axis=1)
        total = nn(put, d_users[...])
        here = block(t, tile_users)
        users_part[here, :width] = total[:, :width] + total[:, width:2 * width]
        users_part[here, width:] = total[:, 2 * width:2 * width + LANES] + total[:, 2 * width + LANES:]
    loop(0, rows // tile_users, sum_users)
    theirs = pl.ds(pl.multiple_of((1 - core) * half, half), half)
    copy(7, users_part.at[theirs], users_part_recv, partner).start()
    wait_recv(7, users_part_recv)
    users_half[...] = (users_part[mine, :] + users_part_recv[...]).astype(BF16)
    tall = nz * BLOCK

    def send_ux(k):
        to = lax.rem(x + k, nx)
        copy(9, users_half.at[block(to, tall)], users_x.at[x], at(z, to, core)).start()
    loop(1, nx, send_ux)

    wait_recv(8, tower_x.at[pl.ds(0, nx - 1)])
    total = tower_part[block(x, wide), :].astype(F32)
    for k in range(1, nx):
        total = total + tower_x[lax.rem(x + k, nx)].astype(F32)
    tower_mid[...] = total.astype(BF16)

    def send_z(k):
        to = lax.rem(z + k, nz)
        copy(10, tower_mid.at[block(to, depth)], tower_z.at[z], at(to, x, core)).start()
    loop(1, nz, send_z)
    far_first(far, nz, send_back)

    wait_recv(13, other_y.at[pl.ds(0, groups - 1)])
    total = other_part[block(g, deep), :].astype(F32)
    for k in range(1, groups):
        total = total + other_y[lax.rem(g + k, groups)].astype(F32)
    other_mid[...] = total.astype(BF16)

    def send_other_x(k):
        to = lax.rem(x + k, nx)
        copy(14, other_mid.at[block(to, depth)], other_x.at[x], at(z, to, core)).start()
    loop(1, nx, send_other_x)

    wait_recv(9, users_x.at[pl.ds(0, nx - 1)])
    total = users_half[block(x, tall), :].astype(F32)
    for k in range(1, nx):
        total = total + users_x[lax.rem(x + k, nx)].astype(F32)
    users_mid[...] = total.astype(BF16)

    def send_uz(k):
        to = lax.rem(z + k, nz)
        copy(11, users_mid.at[block(to, BLOCK)], users_z.at[z], at(to, x, core)).start()
    loop(1, nz, send_uz)

    wait_recv(14, other_x.at[pl.ds(0, nx - 1)])
    total = other_mid[block(x, depth), :].astype(F32)
    for k in range(1, nx):
        total = total + other_x[lax.rem(x + k, nx)].astype(F32)
    other_low[...] = total

    @pl.when(z != g)
    def _():
        copy(15, other_low, other_z.at[z], at(g, x, core)).start()

    wait_recv(10, tower_z.at[pl.ds(0, nz - 1)])
    total = tower_mid[block(z, depth), :].astype(F32)
    for k in range(1, nz):
        total = total + tower_z[lax.rem(z + k, nz)].astype(F32)
    tower_low[...] = total.astype(BF16)

    def send_y(k):
        copy(12, tower_low, tower_y.at[g], (lax.rem(g + k, groups), s)).start()
    loop(1, groups, send_y)

    @pl.when(z == g)
    def _():
        wait_recv(15, other_z.at[pl.ds(0, nz - 1)])
        total = other_low[...]
        for k in range(1, nz):
            total = total + other_z[lax.rem(z + k, nz)]
        other_got[...] = total.astype(BF16)

        def send_other(k):
            copy(16, other_got, other_got, (lax.rem(g + k, groups), s)).start()
        loop(1, groups, send_other)

    wait_recv(6, back_recv.at[pl.ds(0, rows - BLOCK)])
    quarter_row = iota((1, rows), 1) & 3
    for q in range(QUARTERS):
        key = jnp.where(quarter_row == q, asked_row, -1)
        pick = ones_where(key == iota((slots, rows), 0))
        table_out[:, q * width:(q + 1) * width] = nn(pick, back_recv[...])

    wait_recv(11, users_z.at[pl.ds(0, nz - 1)])
    total = users_mid[block(z, BLOCK), :].astype(F32)
    for k in range(1, nz):
        total = total + users_z[lax.rem(z + k, nz)].astype(F32)
    own_rows[...] = total
    for u in range(CAP):
        gate_row = jnp.zeros((1, COMPS * COMPS), F32)
        for q in range(QUARTERS):
            row = u * QUARTERS + q
            users_out[u:u + 1, q * width:(q + 1) * width] = own_rows[row:row + 1, :width]
            gate_row = gate_row + own_rows[row:row + 1, width:width + COMPS * COMPS]
        gates_out[u:u + 1, :] = gate_row

    tower_y[g] = tower_low[...]
    wait_recv(12, tower_y.at[pl.ds(0, groups - 1)])
    total = tower_y[0].astype(F32)
    for k in range(1, groups):
        total = total + tower_y[k].astype(F32)
    tower_out[:, :first] = total

    @pl.when(z != g)
    def _():
        wait_recv(16, other_got)
        wait_send(15, other_low)

    @pl.when(z == g)
    def _():
        wait_send(16, other_part.at[pl.ds(0, (groups - 1) * depth)])

    tower_out[:, first:] = other_got[...].astype(F32)
    wait_send(13, other_y.at[pl.ds(0, groups - 1)])
    wait_send(14, other_x.at[pl.ds(0, nx - 1)])

    wait_send(0, head_send.at[pl.ds(0, shards - 1)])
    wait_send(1, users_all.at[pl.ds(0, direct * BLOCK)])
    if relayed:
        wait_send(19, users_all.at[pl.ds(0, relayed * BLOCK)])
    wait_send(17, gates_all.at[other_gates])
    wait_send(18, gates_all.at[my_gates])
    wait_send(2, xt_recv)
    wait_send(3, rows_send.at[pl.ds(0, rows - BLOCK)])
    wait_send(4, users_all.at[mine])
    wait_send(5, d_pre)
    wait_send(6, back_send.at[pl.ds(0, rows - BLOCK)])
    wait_send(7, users_part_recv)
    wait_send(8, tower_x.at[pl.ds(0, nx - 1)])
    wait_send(9, users_x.at[pl.ds(0, nx - 1)])
    wait_send(10, tower_z.at[pl.ds(0, nz - 1)])
    wait_send(11, users_z.at[pl.ds(0, nz - 1)])
    wait_send(12, tower_y.at[pl.ds(0, groups - 1)])


def local(item_features, tower_weight, item_table, owner, table_slot, pair_users, user_comps, user_gates):
    groups, shards = lax.axis_size("group"), lax.axis_size("shard")
    nx = 4 if shards >= 64 else 2
    nz = shards // (nx * CORES)
    n, d = item_features.shape
    slots = item_table.shape[0]
    held = user_comps.shape[0]
    width = d // QUARTERS
    rows = shards * BLOCK
    half = rows // CORES
    depth = d // shards
    across = width + LANES
    first = d * 5 // 8
    other = d - first
    assert groups == nz
    scratch = [
        ((1, n), jnp.int32), ((1, n), jnp.int32), ((2, n), jnp.int32), ((held, d), BF16), ((held, COMPS * COMPS), BF16),
        ((n, d), BF16), ((d, d), BF16), ((slots, d), BF16),
        ((BLOCK, across), F32), ((BLOCK, width), BF16), ((CAP // 2, 1, LANES), F32), ((shards * CAP // 2, 1, LANES), F32),
        ((shards, 1, LANES), F32), ((shards, 1, LANES), F32),
        ((rows, width), BF16),
        ((CORES, d // 2, n), BF16), ((d // 2, n), BF16),
        ((QUARTERS * n, width), BF16), ((n, d), F32),
        ((rows, width), BF16), ((rows, width), BF16),
        ((2 * QUARTERS * n, width), BF16), ((2 * QUARTERS * n, width), BF16),
        ((QUARTERS * n, width), F32), ((QUARTERS * n, width), BF16),
        ((n, d), BF16), ((n, d), BF16),
        ((2 * QUARTERS * n, 2 * across), BF16), ((2 * QUARTERS * n, 2 * width), BF16),
        ((rows, across), F32), ((half, across), F32),
        ((d // 2, first), BF16), ((nx, nz * depth, first), BF16), ((nz * depth, first), BF16),
        ((nz, depth, first), BF16), ((depth, first), BF16), ((groups, depth, first), BF16),
        ((d // 2, other), BF16), ((groups, nx * depth, other), BF16), ((nx * depth, other), BF16),
        ((nx, depth, other), BF16), ((depth, other), F32), ((nz, depth, other), F32), ((depth, other), BF16),
        ((half, across), BF16), ((nx, nz * BLOCK, across), BF16), ((nz * BLOCK, across), BF16),
        ((nz, BLOCK, across), BF16),
        ((rows, width), BF16), ((rows, width), BF16),
    ]
    whole = pl.BlockSpec(memory_space=pltpu.VMEM)
    return pl.pallas_call(
        functools.partial(kernel, groups, shards, nx),
        out_shape=(
            jax.ShapeDtypeStruct((depth, d), F32),
            jax.ShapeDtypeStruct((slots, d), F32),
            jax.ShapeDtypeStruct((held, d), F32),
            jax.ShapeDtypeStruct((held, COMPS * COMPS), F32),
        ),
        in_specs=[pl.BlockSpec(memory_space=pltpu.HBM)] * 8,
        out_specs=(whole,) * 4,
        scratch_shapes=[pltpu.VMEM(shape, kind) for shape, kind in scratch]
        + [pltpu.SemaphoreType.DMA((20,)), pltpu.SemaphoreType.DMA((20,)), pltpu.SemaphoreType.DMA((nz,)),
           pltpu.SemaphoreType.DMA((8,))],
        compiler_params=pltpu.CompilerParams(
            collective_id=0, has_side_effects=True, vmem_limit_bytes=32 * 1024 * 1024),
    )(*(pltpu.with_memory_space_constraint(a, pltpu.HBM) for a in (
        owner.reshape(1, n), table_slot.reshape(1, n), pair_users.T, user_comps, user_gates,
        item_features, tower_weight, item_table)))


def solution(mesh):
    spread = P(("group", "shard"), None)
    return jax.shard_map(
        local,
        mesh=mesh,
        in_specs=(spread, P(), spread, spread, P(("group", "shard")), spread, spread, spread),
        out_specs=(P("shard", None), spread, spread, spread),
        check_vma=False,
    )
```

```python
import functools

import jax
import jax.numpy as jnp
from jax import lax
from jax.experimental import pallas as pl
from jax.experimental.pallas import tpu as pltpu
from jax.sharding import PartitionSpec as P

MESH = pl.DeviceIdType.MESH
COMPS = 8
CAP = 4
CORES = 2
QUARTERS = 4
BLOCK = CAP * QUARTERS
GROUP = 16
LANES = 128
F32, BF16 = jnp.float32, jnp.bfloat16


def nn(a, b):
    return lax.dot_general(a, b, (((1,), (0,)), ((), ())), preferred_element_type=F32)


def nt(a, b):
    return lax.dot_general(a, b, (((1,), (1,)), ((), ())), preferred_element_type=F32)


def tn(a, b):
    return lax.dot_general(a, b, (((0,), (0,)), ((), ())), preferred_element_type=F32)


def ones_where(condition):
    return jnp.where(condition, 1.0, 0.0).astype(BF16)


def iota(shape, dim):
    return lax.broadcasted_iota(jnp.int32, shape, dim)


def halves(values):
    high = values.astype(BF16)
    return high, (values - high.astype(F32)).astype(BF16)


def sigmoid(values):
    return 1.0 / (1.0 + jnp.exp(-values))


def kernel(
    groups, shards, nx,
    owner_hbm, slot_hbm, pair_hbm, comps_hbm, gates_hbm, x_hbm, w_hbm, table_hbm,
    tower_out, table_out, users_out, gates_out,
    owner_ref, slot_ref, pair_ref, comps_ref, gates_ref, x_ref, w_ref, table_ref,
    own_rows, own_users, own_gates, gates_all, head_send, head_recv, users_all, xt, xt_recv, embedded, slope, rows_send, rows_recv,
    picked, gates_wide, combined, d_comb, d_pre, d_pre_recv, d_users, d_gates,
    users_part, users_part_recv, tower_part, tower_x, tower_mid, tower_z, tower_low, tower_y,
    other_part, other_y, other_mid, other_x, other_low, other_z, other_got,
    users_half, users_x, users_mid, users_z, back_send, back_recv,
    send_sems, recv_sems, head_sems, load_sems,
):
    n, d = x_ref.shape
    slots = table_ref.shape[0]
    width = d // QUARTERS
    rows = shards * BLOCK
    half = rows // CORES
    nz = shards // (nx * CORES)
    depth = d // shards
    chips = shards // CORES
    g, s = lax.axis_index("group"), lax.axis_index("shard")
    core = lax.rem(s, CORES)
    chip = lax.div(s, CORES)
    x, z = lax.rem(chip, nx), lax.div(chip, nx)

    def at(z_to, x_to, core_to):
        return (g, (z_to * nx + x_to) * CORES + core_to)

    partner = at(z, x, 1 - core)

    def copy(number, source, target, device):
        return pltpu.make_async_remote_copy(
            src_ref=source, dst_ref=target,
            send_sem=send_sems.at[number], recv_sem=recv_sems.at[number],
            device_id=device, device_id_type=MESH,
        )

    def wait_recv(number, whole):
        copy(number, whole, whole, partner).wait_recv()

    def wait_send(number, whole):
        copy(number, whole, whole, partner).wait_send()

    def loop(low, high, step):
        def run(i, carry):
            step(i)
            return carry
        lax.fori_loop(low, high, run, 0)

    def block(i, size):
        return pl.ds(pl.multiple_of(i * size, size), size)

    loads = [
        pltpu.make_async_copy(source, target, load_sems.at[i])
        for i, (source, target) in enumerate((
            (owner_hbm, owner_ref), (slot_hbm, slot_ref), (pair_hbm, pair_ref), (comps_hbm, comps_ref),
            (gates_hbm, gates_ref), (x_hbm, x_ref), (w_hbm, w_ref), (table_hbm, table_ref)))
    ]
    for load in loads:
        load.start()
    barrier = pltpu.get_barrier_semaphore()
    loop(1, shards, lambda k: pl.semaphore_signal(
        barrier, inc=1, device_id=(g, lax.rem(s + k, shards)), device_id_type=MESH))
    loop(1, groups, lambda k: pl.semaphore_signal(
        barrier, inc=1, device_id=(lax.rem(g + k, groups), s), device_id_type=MESH))

    for load in loads[:5]:
        load.wait()

    target = owner_ref[...]
    slot = slot_ref[...]
    to_owner = jnp.where(iota((shards, n), 0) == target, 1.0, 0.0)
    earlier = ones_where(iota((n, n), 0) < iota((n, n), 1))
    before = nn(to_owner.astype(BF16), earlier)
    within = jnp.sum(before * to_owner, axis=0, keepdims=True).astype(jnp.int32)
    place_row = (target * CAP + within) * QUARTERS
    eye = iota((n, n), 0) == iota((n, n), 1)

    def as_column(row):
        wide = jnp.where(eye, row.astype(F32), 0.0)
        return jnp.sum(wide, axis=1, keepdims=True).astype(jnp.int32)

    place_col = as_column(place_row)
    wanted = (to_owner * (slot + 1).astype(F32)).astype(BF16)
    turn = ones_where(iota((LANES, n), 0) == within)
    head_send[...] = nt(wanted, turn).reshape(shards, 1, LANES)

    own_comps, gate_values = comps_ref[...].astype(F32), gates_ref[...].astype(F32)
    for u in range(CAP):
        for q in range(QUARTERS):
            row = u * QUARTERS + q
            own_rows[row:row + 1, :width] = own_comps[u:u + 1, q * width:(q + 1) * width]
    own_users[...] = own_rows[:, :width].astype(BF16)
    for pair in range(CAP // 2):
        own_gates[pair] = jnp.concatenate([gate_values[2 * pair:2 * pair + 1], gate_values[2 * pair + 1:2 * pair + 2]], axis=1)
    own = core * chips + x * nz + z
    users_all[block(own, BLOCK), :] = own_users[...]
    gate_rows = CAP // 2
    gates_all[pl.ds(own * gate_rows, gate_rows)] = own_gates[...]

    pl.semaphore_wait(barrier, shards - 1 + groups - 1)

    column = nx * CORES

    def head(away, p):
        return pltpu.make_async_remote_copy(
            src_ref=head_send.at[p], dst_ref=head_recv.at[s],
            send_sem=send_sems.at[0], recv_sem=head_sems.at[away],
            device_id=(g, p), device_id_type=MESH,
        )

    def send_head(k):
        p = lax.rem(s + k, shards)
        head(lax.rem(z - lax.div(p, column) + nz, nz), p).start()
    loop(1, shards, send_head)
    head_recv[s] = head_send[s]

    def send_users(k):
        p = lax.rem(chip + k, chips)
        copy(1, own_users, users_all.at[block(own, BLOCK)], (g, p * CORES + core)).start()
        copy(17, own_gates, gates_all.at[pl.ds(own * gate_rows, gate_rows)], (g, p * CORES + core)).start()
    loop(1, chips, send_users)
    loads[5].wait()

    for tile in range(d // LANES):
        turned = x_ref[:, tile * LANES:(tile + 1) * LANES].astype(F32).T.astype(BF16)
        for piece in range(max(1, LANES // depth)):
            size = min(depth, LANES)
            first = tile * LANES + piece * size
            holder, rest = divmod(first, depth)
            c_h, chip_h = holder % CORES, holder // CORES
            row = ((chip_h % nx) * nz + chip_h // nx) * depth + rest
            xt[c_h, row:row + size, :] = turned[piece * size:(piece + 1) * size]

    copy(2, xt.at[1 - core], xt_recv, partner).start()

    loads[6].wait()

    def tower(q):
        columns = block(q, width)
        pre = nn(x_ref[...], w_ref[:, columns])
        share = 0.5 + 0.5 * lax.erf(pre * (0.5 ** 0.5))
        embedded[block(q, n), :] = (pre * share).astype(BF16)
        slope[:, columns] = share + pre * (0.3989422804014327 * jnp.exp(-0.5 * pre * pre))
    loop(0, QUARTERS, tower)

    tile_rows = min(256, rows)
    span = column * BLOCK

    def answer(step):
        away = (step + 1) >> 1
        off = jnp.where((step & 1) == 1, away, nz - away)
        z_from = lax.rem(z + off, nz)
        first = z_from * column

        @pl.when(step == 0)
        def _():
            pltpu.make_async_copy(
                head_recv.at[pl.ds(0, column - 1)], head_recv.at[pl.ds(0, column - 1)], head_sems.at[0]).wait()

        @pl.when(step > 0)
        def _():
            whole = head_recv.at[pl.ds(0, column)]
            pltpu.make_async_copy(whole, whole, head_sems.at[lax.rem(off, nz)]).wait()

        heads = head_recv[pl.ds(first, column)].reshape(column, LANES).astype(BF16)
        spread = nn(ones_where((iota((span, column), 0) >> 4) == iota((span, column), 1)), heads)
        index = iota((span, LANES), 0)
        mine = jnp.where(((index >> 2) & 3) == iota((span, LANES), 1), spread, 0.0)
        asked = jnp.sum(mine, axis=1, keepdims=True).astype(jnp.int32) - 1
        quarter = index[:, 0:1] & 3
        out = jnp.zeros((span, width), F32)
        for q in range(QUARTERS):
            key = jnp.where(quarter == q, asked, -1)
            pick = ones_where(key == iota((span, slots), 1))
            out = out + nn(pick, table_ref[:, q * width:(q + 1) * width])
        rows_send[block(z_from, span), :] = out.astype(BF16)

        def send_rows(k):
            p = first + k

            @pl.when(p != s)
            def _():
                copy(3, rows_send.at[block(p, BLOCK)], rows_recv.at[block(s, BLOCK)], (g, p)).start()
        loop(0, column, send_rows)
    loads[7].wait()
    loop(0, nz, answer)
    rows_recv[block(s, BLOCK), :] = rows_send[block(s, BLOCK), :]

    others = pl.ds(0, half - BLOCK)
    wait_recv(1, users_all.at[others])
    mine = pl.ds(pl.multiple_of(core * half, half), half)
    copy(4, users_all.at[mine], users_all.at[mine], partner).start()
    other_gates = pl.ds(0, (chips - 1) * gate_rows)
    wait_recv(17, gates_all.at[other_gates])
    my_gates = pl.ds(core * chips * gate_rows, chips * gate_rows)
    copy(18, gates_all.at[my_gates], gates_all.at[my_gates], partner).start()

    heads = head_recv[...].reshape(shards, LANES).astype(BF16)
    held = tn(heads, ones_where((iota((shards, rows), 1) >> 4) == iota((shards, rows), 0)))
    lane = iota((LANES, rows), 1)
    held = jnp.where(((lane >> 2) & 3) == iota((LANES, rows), 0), held, 0.0)
    asked_row = jnp.sum(held, axis=0, keepdims=True).astype(jnp.int32) - 1

    def user_key(row):
        user, holder = row & 3, row >> 2
        c_u, chip_u = holder & 1, holder >> 1
        where = c_u * chips + (chip_u & (nx - 1)) * nz + (chip_u >> (nx.bit_length() - 1))
        return (where * CAP + user) * QUARTERS

    key_rows = [user_key(pair_ref[side:side + 1, :]) for side in range(2)]
    key_cols = [as_column(row) for row in key_rows]
    gate = iota((LANES, width), 0)
    expand = ones_where((gate < COMPS * COMPS) & ((gate & 15) == (iota((LANES, width), 1) >> 4)))
    wait_recv(4, users_all.at[mine])
    wait_recv(18, gates_all.at[my_gates])
    gate_table = gates_all[...].reshape(shards * gate_rows, LANES).astype(BF16)
    gate_lane = iota((LANES, width), 0)
    gate_of = (gate_lane & 15) == (iota((LANES, width), 1) >> 4)
    for side in range(2):
        user = key_cols[side] >> 2
        taken = nn(ones_where((user >> 1) == iota((n, shards * gate_rows), 1)), gate_table)
        taken = jnp.where((iota((n, LANES), 1) >> 6) == (user & 1), taken, 0.0).astype(BF16)

        def pick_users(q):
            pick = ones_where(key_cols[side] + q == iota((n, rows), 1))
            here = block(side * QUARTERS + q, n)
            picked[here, :] = nn(pick, users_all[...]).astype(BF16)
            part = ones_where(gate_of & (((gate_lane & 63) >> 4) == q))
            gates_wide[here, :] = nn(taken, part).astype(BF16)
        loop(0, QUARTERS, pick_users)

    wait_recv(3, rows_recv.at[pl.ds(0, rows - BLOCK)])

    def combine(q):
        pick = ones_where(place_col + q == iota((n, rows), 1))
        here = block(q, n)
        combined[here, :] = embedded[here, :].astype(F32) + nn(pick, rows_recv[...])
    loop(0, QUARTERS, combine)

    def spot(index, b):
        return pl.ds(pl.multiple_of(index * n + b * GROUP, GROUP), GROUP)

    def lanes_of(p):
        return slice((p & 1) * LANES, (p & 1) * LANES + LANES)

    def stack(ref, b, sides):
        return jnp.concatenate(
            [ref[spot(side * QUARTERS + (p >> 1), b), lanes_of(p)] for side in range(sides) for p in range(COMPS)],
            axis=0)

    pairs = COMPS * GROUP

    def pair_loss(b):
        stores = []

        def store(ref, where, lanes, values):
            stores.append((ref, where, lanes, values))

        comb = stack(combined, b, 1)
        scale = lax.rsqrt(jnp.mean(comb * comb, axis=1, keepdims=True) + 1e-06)
        normed = comb * scale
        n_high, n_low = halves(normed)
        users = stack(picked, b, 2)
        gates = stack(gates_wide, b, 2).astype(F32)
        logits = nt(users, n_high) + nt(users, n_low)
        same = (iota((2 * pairs, pairs), 0) & (GROUP - 1)) == (iota((2 * pairs, pairs), 1) & (GROUP - 1))
        weights = sigmoid(gates + logits)
        terms = jnp.where(same, weights * logits, 0.0)
        factors = []
        for side in range(2):
            total = terms[side * pairs:side * pairs + GROUP]
            for p in range(1, COMPS):
                total = total + terms[side * pairs + p * GROUP:side * pairs + (p + 1) * GROUP]
            score = 0.125 * jnp.sum(total, axis=1, keepdims=True)
            factor = sigmoid(score) if side else -sigmoid(-score)
            factors += [0.125 * factor] * COMPS
        factor = jnp.where(same, jnp.concatenate(factors, axis=0), 0.0)
        bend = logits * (weights * (1.0 - weights))
        dg_high, dg_low = halves(factor * bend)
        dl = factor * (weights + bend)
        dl_high, dl_low = halves(dl)
        d_normed = tn(dl_high, users) + tn(dl_low, users)
        du_high, du_low = halves(nn(dl_high, n_high) + nn(dl_low, n_high) + nn(dl_high, n_low))
        d_row = scale * (d_normed - normed * jnp.mean(d_normed * normed, axis=1, keepdims=True))
        d_row = d_row.astype(BF16)
        for p in range(COMPS):
            part = d_row[p * GROUP:(p + 1) * GROUP]
            store(d_comb, spot(p >> 1, b), lanes_of(p), part)
            item, column = block(b, GROUP), slice(p * LANES, (p + 1) * LANES)
            store(d_pre, item, column, (part.astype(F32) * slope[item, column]).astype(BF16))
        for side in range(2):
            for p in range(COMPS):
                here = spot(side * QUARTERS + (p >> 1), b)
                part = slice(side * pairs + p * GROUP, side * pairs + (p + 1) * GROUP)
                lane0 = (p & 1) * LANES
                store(d_users, here, slice(lane0, lane0 + LANES), du_high[part])
                store(d_users, here, slice(width + lane0, width + lane0 + LANES), du_low[part])
                store(d_gates, here, slice(lane0, lane0 + LANES), dg_high[part])
                store(d_gates, here, slice(width + lane0, width + lane0 + LANES), dg_low[part])
        return stores

    together = 2 - (n // GROUP) % 2

    def pair_losses(t):
        for stores in [pair_loss(t * together + i) for i in range(together)]:
            for ref, where, lanes, values in stores:
                ref[where, lanes] = values
    loop(0, n // (GROUP * together), pair_losses)

    copy(5, d_pre, d_pre_recv, partner).start()

    def give_back(t):
        index = iota((tile_rows, n), 0) + t * tile_rows
        put = jnp.concatenate([ones_where(index == place_row + q) for q in range(QUARTERS)], axis=1)
        back_send[block(t, tile_rows), :] = nn(put, d_comb[...]).astype(BF16)
    loop(0, rows // tile_rows, give_back)

    first = tower_part.shape[1]
    deep = nx * depth
    wait_recv(2, xt_recv)
    wait_recv(5, d_pre_recv)
    wide = nz * depth

    def tower_rows(i):
        here = block(i, wide)
        total = nn(xt[core, here, :], d_pre[...]) + nn(xt_recv[here, :], d_pre_recv[...])
        tower_part[here, :] = total[:, :first].astype(BF16)
        for j in range(nz):
            there = pl.ds(pl.multiple_of((j * nx + i) * depth, depth), depth)
            other_part[there, :] = total[j * depth:(j + 1) * depth, first:].astype(BF16)
    loop(0, nx, tower_rows)

    def send_x(k):
        to = lax.rem(x + k, nx)
        copy(8, tower_part.at[block(to, wide)], tower_x.at[x], at(z, to, core)).start()
    loop(1, nx, send_x)

    def send_other_y(k):
        to = lax.rem(g + k, groups)
        copy(13, other_part.at[block(to, deep)], other_y.at[g], (to, s)).start()
    loop(1, groups, send_other_y)

    far = max(1, 3 * nz // 8)

    def send_back(step):
        away = (step + 1) >> 1
        z_to = lax.rem(z + nz // 2 + jnp.where((step & 1) == 1, nz - away, away), nz)

        def send_one(k):
            p = z_to * column + k

            @pl.when(p != s)
            def _():
                copy(6, back_send.at[block(p, BLOCK)], back_recv.at[block(s, BLOCK)], (g, p)).start()
        loop(0, column, send_one)
    loop(0, far, send_back)
    back_recv[block(s, BLOCK), :] = back_send[block(s, BLOCK), :]

    def squeeze(i):
        here = block(i, n)
        high, low = halves(nt(d_gates[here, :width], expand) + nt(d_gates[here, width:], expand))
        ours = (iota((n, LANES), 1) >> 4) == (i & 3)
        zero = jnp.zeros((n, LANES), BF16)
        d_users[here, 2 * width:2 * width + LANES] = jnp.where(ours, high, zero)
        d_users[here, 2 * width + LANES:] = jnp.where(ours, low, zero)
    loop(0, 2 * QUARTERS, squeeze)

    tile_users = min(128, rows)

    def sum_users(t):
        index = iota((tile_users, n), 0) + t * tile_users
        put = jnp.concatenate(
            [ones_where(index == key_rows[side] + q) for side in range(2) for q in range(QUARTERS)], axis=1)
        total = nn(put, d_users[...])
        here = block(t, tile_users)
        users_part[here, :width] = total[:, :width] + total[:, width:2 * width]
        users_part[here, width:] = total[:, 2 * width:2 * width + LANES] + total[:, 2 * width + LANES:]
    loop(0, rows // tile_users, sum_users)
    theirs = pl.ds(pl.multiple_of((1 - core) * half, half), half)
    copy(7, users_part.at[theirs], users_part_recv, partner).start()
    wait_recv(7, users_part_recv)
    users_half[...] = (users_part[mine, :] + users_part_recv[...]).astype(BF16)
    tall = nz * BLOCK

    def send_ux(k):
        to = lax.rem(x + k, nx)
        copy(9, users_half.at[block(to, tall)], users_x.at[x], at(z, to, core)).start()
    loop(1, nx, send_ux)

    wait_recv(8, tower_x.at[pl.ds(0, nx - 1)])
    total = tower_part[block(x, wide), :].astype(F32)
    for k in range(1, nx):
        total = total + tower_x[lax.rem(x + k, nx)].astype(F32)
    tower_mid[...] = total.astype(BF16)

    def send_z(k):
        to = lax.rem(z + k, nz)
        copy(10, tower_mid.at[block(to, depth)], tower_z.at[z], at(to, x, core)).start()
    loop(1, nz, send_z)
    loop(far, nz, send_back)

    wait_recv(13, other_y.at[pl.ds(0, groups - 1)])
    total = other_part[block(g, deep), :].astype(F32)
    for k in range(1, groups):
        total = total + other_y[lax.rem(g + k, groups)].astype(F32)
    other_mid[...] = total.astype(BF16)

    def send_other_x(k):
        to = lax.rem(x + k, nx)
        copy(14, other_mid.at[block(to, depth)], other_x.at[x], at(z, to, core)).start()
    loop(1, nx, send_other_x)

    wait_recv(9, users_x.at[pl.ds(0, nx - 1)])
    total = users_half[block(x, tall), :].astype(F32)
    for k in range(1, nx):
        total = total + users_x[lax.rem(x + k, nx)].astype(F32)
    users_mid[...] = total.astype(BF16)

    def send_uz(k):
        to = lax.rem(z + k, nz)
        copy(11, users_mid.at[block(to, BLOCK)], users_z.at[z], at(to, x, core)).start()
    loop(1, nz, send_uz)

    wait_recv(14, other_x.at[pl.ds(0, nx - 1)])
    total = other_mid[block(x, depth), :].astype(F32)
    for k in range(1, nx):
        total = total + other_x[lax.rem(x + k, nx)].astype(F32)
    other_low[...] = total

    @pl.when(z != g)
    def _():
        copy(15, other_low, other_z.at[z], at(g, x, core)).start()

    wait_recv(10, tower_z.at[pl.ds(0, nz - 1)])
    total = tower_mid[block(z, depth), :].astype(F32)
    for k in range(1, nz):
        total = total + tower_z[lax.rem(z + k, nz)].astype(F32)
    tower_low[...] = total.astype(BF16)

    def send_y(k):
        copy(12, tower_low, tower_y.at[g], (lax.rem(g + k, groups), s)).start()
    loop(1, groups, send_y)

    @pl.when(z == g)
    def _():
        wait_recv(15, other_z.at[pl.ds(0, nz - 1)])
        total = other_low[...]
        for k in range(1, nz):
            total = total + other_z[lax.rem(z + k, nz)]
        other_got[...] = total.astype(BF16)

        def send_other(k):
            copy(16, other_got, other_got, (lax.rem(g + k, groups), s)).start()
        loop(1, groups, send_other)

    wait_recv(6, back_recv.at[pl.ds(0, rows - BLOCK)])
    quarter_row = iota((1, rows), 1) & 3
    for q in range(QUARTERS):
        key = jnp.where(quarter_row == q, asked_row, -1)
        pick = ones_where(key == iota((slots, rows), 0))
        table_out[:, q * width:(q + 1) * width] = nn(pick, back_recv[...])

    wait_recv(11, users_z.at[pl.ds(0, nz - 1)])
    total = users_mid[block(z, BLOCK), :].astype(F32)
    for k in range(1, nz):
        total = total + users_z[lax.rem(z + k, nz)].astype(F32)
    own_rows[...] = total
    for u in range(CAP):
        gate_row = jnp.zeros((1, COMPS * COMPS), F32)
        for q in range(QUARTERS):
            row = u * QUARTERS + q
            users_out[u:u + 1, q * width:(q + 1) * width] = own_rows[row:row + 1, :width]
            gate_row = gate_row + own_rows[row:row + 1, width:width + COMPS * COMPS]
        gates_out[u:u + 1, :] = gate_row

    tower_y[g] = tower_low[...]
    wait_recv(12, tower_y.at[pl.ds(0, groups - 1)])
    total = tower_y[0].astype(F32)
    for k in range(1, groups):
        total = total + tower_y[k].astype(F32)
    tower_out[:, :first] = total

    @pl.when(z != g)
    def _():
        wait_recv(16, other_got)
        wait_send(15, other_low)

    @pl.when(z == g)
    def _():
        wait_send(16, other_part.at[pl.ds(0, (groups - 1) * depth)])

    tower_out[:, first:] = other_got[...].astype(F32)
    wait_send(13, other_y.at[pl.ds(0, groups - 1)])
    wait_send(14, other_x.at[pl.ds(0, nx - 1)])

    wait_send(0, head_send.at[pl.ds(0, shards - 1)])
    wait_send(1, users_all.at[others])
    wait_send(17, gates_all.at[other_gates])
    wait_send(18, gates_all.at[my_gates])
    wait_send(2, xt_recv)
    wait_send(3, rows_send.at[pl.ds(0, rows - BLOCK)])
    wait_send(4, users_all.at[mine])
    wait_send(5, d_pre)
    wait_send(6, back_send.at[pl.ds(0, rows - BLOCK)])
    wait_send(7, users_part_recv)
    wait_send(8, tower_x.at[pl.ds(0, nx - 1)])
    wait_send(9, users_x.at[pl.ds(0, nx - 1)])
    wait_send(10, tower_z.at[pl.ds(0, nz - 1)])
    wait_send(11, users_z.at[pl.ds(0, nz - 1)])
    wait_send(12, tower_y.at[pl.ds(0, groups - 1)])


def local(item_features, tower_weight, item_table, owner, table_slot, pair_users, user_comps, user_gates):
    groups, shards = lax.axis_size("group"), lax.axis_size("shard")
    nx = 4 if shards >= 64 else 2
    nz = shards // (nx * CORES)
    n, d = item_features.shape
    slots = item_table.shape[0]
    held = user_comps.shape[0]
    width = d // QUARTERS
    rows = shards * BLOCK
    half = rows // CORES
    depth = d // shards
    across = width + LANES
    first = d // 2
    other = d - first
    assert groups == nz
    scratch = [
        ((1, n), jnp.int32), ((1, n), jnp.int32), ((2, n), jnp.int32), ((held, d), BF16), ((held, COMPS * COMPS), BF16),
        ((n, d), BF16), ((d, d), BF16), ((slots, d), BF16),
        ((BLOCK, across), F32), ((BLOCK, width), BF16), ((CAP // 2, 1, LANES), F32), ((shards * CAP // 2, 1, LANES), F32),
        ((shards, 1, LANES), F32), ((shards, 1, LANES), F32),
        ((rows, width), BF16),
        ((CORES, d // 2, n), BF16), ((d // 2, n), BF16),
        ((QUARTERS * n, width), BF16), ((n, d), F32),
        ((rows, width), BF16), ((rows, width), BF16),
        ((2 * QUARTERS * n, width), BF16), ((2 * QUARTERS * n, width), BF16),
        ((QUARTERS * n, width), F32), ((QUARTERS * n, width), BF16),
        ((n, d), BF16), ((n, d), BF16),
        ((2 * QUARTERS * n, 2 * across), BF16), ((2 * QUARTERS * n, 2 * width), BF16),
        ((rows, across), F32), ((half, across), F32),
        ((d // 2, first), BF16), ((nx, nz * depth, first), BF16), ((nz * depth, first), BF16),
        ((nz, depth, first), BF16), ((depth, first), BF16), ((groups, depth, first), BF16),
        ((d // 2, other), BF16), ((groups, nx * depth, other), BF16), ((nx * depth, other), BF16),
        ((nx, depth, other), BF16), ((depth, other), F32), ((nz, depth, other), F32), ((depth, other), BF16),
        ((half, across), BF16), ((nx, nz * BLOCK, across), BF16), ((nz * BLOCK, across), BF16),
        ((nz, BLOCK, across), BF16),
        ((rows, width), BF16), ((rows, width), BF16),
    ]
    whole = pl.BlockSpec(memory_space=pltpu.VMEM)
    return pl.pallas_call(
        functools.partial(kernel, groups, shards, nx),
        out_shape=(
            jax.ShapeDtypeStruct((depth, d), F32),
            jax.ShapeDtypeStruct((slots, d), F32),
            jax.ShapeDtypeStruct((held, d), F32),
            jax.ShapeDtypeStruct((held, COMPS * COMPS), F32),
        ),
        in_specs=[pl.BlockSpec(memory_space=pltpu.HBM)] * 8,
        out_specs=(whole,) * 4,
        scratch_shapes=[pltpu.VMEM(shape, kind) for shape, kind in scratch]
        + [pltpu.SemaphoreType.DMA((19,)), pltpu.SemaphoreType.DMA((19,)), pltpu.SemaphoreType.DMA((nz,)),
           pltpu.SemaphoreType.DMA((8,))],
        compiler_params=pltpu.CompilerParams(
            collective_id=0, has_side_effects=True, vmem_limit_bytes=32 * 1024 * 1024),
    )(*(pltpu.with_memory_space_constraint(a, pltpu.HBM) for a in (
        owner.reshape(1, n), table_slot.reshape(1, n), pair_users.T, user_comps, user_gates,
        item_features, tower_weight, item_table)))


def solution(mesh):
    spread = P(("group", "shard"), None)
    return jax.shard_map(
        local,
        mesh=mesh,
        in_specs=(spread, P(), spread, spread, P(("group", "shard")), spread, spread, spread),
        out_specs=(P("shard", None), spread, spread, spread),
        check_vma=False,
    )
```
